32 devices in a mesh: gx: 8 (over z, x), gy: 4 (over y, core).
Axes of the slice: x: 2, y: 2, z: 4, core: 2. Of those that a mesh axis runs over, the one named last changes fastest.
Arguments:
- pooled: bfloat16 [4096, 8, 128], P(('gx', 'gy')), may hold values from -6 to 6
- cotangent: bfloat16 [4096, 28, 128], P(('gx', 'gy')), may hold values from -0.09375 to 0.09375
- bilinear: bfloat16 [7, 128, 128], replicated, may hold values from -0.5 to 0.5
- bag_ids: int32 [4096, 8, 4], P(('gx', 'gy')), may hold values from 0 to 8191, as said below
- bag_lens: int32 [4096, 8], P(('gx', 'gy')), may hold values from 1 to 4
- row_home: int32 [8, 8192], replicated, may hold values from 0 to 8191, as said below
Outputs:
- weight_grad: float32 [7, 128, 128], replicated
- table_grad: float32 [8192, 8, 128], P(('gx', 'gy'))
The draws below stay inside these ranges and needn't reach their ends.
Inputs may be any that keep to these rules, and one draw needn't show every extreme that they name: Each row row_home[f] is a permutation; row r of field f's table is stored at position row_home[f, r] of table_grad's first dimension. Only the first bag_lens entries of a bag are live. The stored position q = row_home[f, bag_ids[sample, f, k]] of an entry lies in the block of 256 positions of device q // 256 (devices in gx+gy order); among all entries of one device's samples, live or not, at most 256 lie in any one device's block; in every device's entries some block is hit exactly 256 times, and one block is hit exactly 256 times by the entries of every device.
All inputs are finite; a program needn't handle non-finite values.
Results may differ from the reference program's by a relative error of at most 0.0035.
Values may be sent and summed in bfloat16 or wider, within the bound.
A program may use at most 64 MiB of HBM per device.

```python
import jax
import jax.numpy as jnp
from jax import lax

D = 128
FIELDS = 8
PAIRS = 28
BAG = 4
TOK_DEV = 128
R_DEV = 256
TOKENS = 4096
ROWS = 8192
CAP = 256
N_GX = 8
N_GY = 4


def home_table(key):
    field_keys = jax.random.split(jax.random.fold_in(key, 101), FIELDS)
    return jax.vmap(lambda k: jax.random.permutation(k, ROWS))(field_keys).astype(jnp.int32)


def draw_row_home(key, part):
    return home_table(key)


def draw_bag_ids(key, part):
    home = home_table(key)
    inverse = jnp.argsort(home, axis=1, stable=True).astype(jnp.int32)
    owners_all = N_GX * N_GY
    slots = CAP * owners_all
    entries = TOK_DEV * FIELDS * BAG
    route_key = jax.random.fold_in(key, 202)
    hotness = jax.random.randint(jax.random.fold_in(route_key, 1), (owners_all,), 0, 4).astype(jnp.int32)
    shared_full = jax.random.randint(jax.random.fold_in(route_key, 2), (), 0, owners_all).astype(jnp.int32)
    slot_owner = (jnp.arange(slots, dtype=jnp.int32) // CAP).astype(jnp.int32)

    def one_block(block):
        block_key = jax.random.fold_in(route_key, 1000 + block)
        raw = jax.random.randint(jax.random.fold_in(block_key, 1), (slots,), 0, 4096).astype(jnp.int32)
        score = jnp.right_shift(raw, 2 * hotness[slot_owner])
        own_full = jax.random.randint(jax.random.fold_in(block_key, 2), (), 0, owners_all).astype(jnp.int32)
        forced = jnp.logical_or(slot_owner == own_full, slot_owner == shared_full)
        score = jnp.where(forced, -1, score)
        rank_key = score * slots + jnp.arange(slots, dtype=jnp.int32)
        picked = jnp.argsort(rank_key, stable=True)[:entries]
        owners = slot_owner[picked]
        owners = owners[jax.random.permutation(jax.random.fold_in(block_key, 3), entries)]
        first = jax.random.randint(jax.random.fold_in(block_key, 4), (entries,), 0, R_DEV).astype(jnp.int32)
        second = jax.random.randint(jax.random.fold_in(block_key, 5), (entries,), 0, R_DEV).astype(jnp.int32)
        local = first * second // R_DEV
        return (owners * R_DEV + local).astype(jnp.int32)
    stored = lax.map(one_block, jnp.arange(owners_all, dtype=jnp.int32)).reshape(TOKENS, FIELDS, BAG)
    field_index = jnp.arange(FIELDS, dtype=jnp.int32)[None, :, None]
    return inverse[field_index, stored].astype(jnp.int32)


def plant(result, key, low, high):
    spot = [jax.random.randint(jax.random.fold_in(key, axis), (), 0, length) for axis, length in enumerate(result.shape)]
    widest = result.shape.index(max(result.shape))
    beside = spot[:widest] + [(spot[widest] + 1) % result.shape[widest]] + spot[widest + 1:]
    return result.at[tuple(spot)].set(low).at[tuple(beside)].set(high)


def steps_of(stream_key, extent, cuts, smallest, largest):
    gain = 1.0
    for axis_at, blocks in cuts:
        draws = jax.random.uniform(jax.random.fold_in(jax.random.fold_in(stream_key, 6), axis_at), (blocks,), jnp.float32, smallest / len(cuts), largest / len(cuts))
        gain = gain * jnp.repeat(jnp.exp(draws), extent[axis_at] // blocks).reshape((-1,) + (1,) * (len(extent) - 1 - axis_at))
    return gain


def scatter_about(key, shape, width, most, shards=(), held_as=jnp.bfloat16):
    level = steps_of(key, shape, shards, -0.22, 0.18) if shards else 1.0
    result = jax.random.normal(key, shape, jnp.float32) * width * level
    return jnp.minimum(jnp.maximum(result, -most), most).astype(held_as)


def setup_inputs(seed: int = 0) -> dict:
    key_of = jax.random.split(jax.random.key(seed), 7)
    return {
        "pooled": scatter_about(key_of[0], (TOKENS, FIELDS, D), 1.0, 6.0, ((0, 32),)),
        "cotangent": scatter_about(key_of[1], (TOKENS, PAIRS, D), TOKENS ** -0.5, 0.09375, ((0, 32),)),
        "bilinear": scatter_about(key_of[2], (FIELDS - 1, D, D), D ** -0.5, 0.5),
        "bag_ids": draw_bag_ids(jax.random.fold_in(key_of[6], 71), 0),
        "bag_lens": plant(jax.random.randint(key_of[4], (TOKENS, FIELDS), 1, BAG + 1), jax.random.fold_in(key_of[4], 1), 1, BAG).astype(jnp.int32),
        "row_home": draw_row_home(jax.random.fold_in(key_of[6], 71), 0),
    }


def pair_list(fields):
    return [(i, j) for i in range(fields) for j in range(i + 1, fields)]


def reference(pooled, cotangent, bilinear, bag_ids, bag_lens, row_home):
    pair_order = pair_list(FIELDS)
    embedded = pooled.astype(jnp.float32)
    weights = bilinear.astype(jnp.float32)
    cot_rows = cotangent.astype(jnp.float32)
    projected = jnp.einsum('bfd,fde->bfe', embedded[:, :FIELDS - 1], weights)
    upper_terms = []
    for i in range(FIELDS - 1):
        running = jnp.zeros((TOKENS, D), jnp.float32)
        for p, (a, c) in enumerate(pair_order):
            if a == i:
                running = running + cot_rows[:, p] * embedded[:, c]
        upper_terms.append(running)
    upper_bf = jnp.stack(upper_terms, 1).astype(jnp.bfloat16).astype(jnp.float32)
    weight_grad = jnp.einsum('bfd,bfe->fde', embedded[:, :FIELDS - 1], upper_bf)
    field_list = []
    for i in range(FIELDS):
        running = jnp.zeros((TOKENS, D), jnp.float32)
        if i < FIELDS - 1:
            running = running + jnp.einsum('be,de->bd', upper_bf[:, i], weights[i])
        for p, (a, c) in enumerate(pair_order):
            if c == i:
                running = running + cot_rows[:, p] * projected[:, a]
        field_list.append(running)
    field_grads = jnp.stack(field_list, 1).astype(jnp.bfloat16).astype(jnp.float32)
    live = jnp.arange(BAG, dtype=jnp.int32)[None, :]
    tables = []
    for f in range(FIELDS):
        stored = row_home[f][bag_ids[:, f, :]]
        segment = jnp.where(live < bag_lens[:, f, None], stored, ROWS).astype(jnp.int32)
        values = jnp.broadcast_to(field_grads[:, f, None, :], (TOKENS, BAG, D)).reshape(TOKENS * BAG, D)
        summed = jax.ops.segment_sum(values, segment.reshape(-1), num_segments=ROWS + 1)
        tables.append(summed[:ROWS])
    return weight_grad, jnp.stack(tables, 1)
```

```python
import functools
import math

import jax
import jax.numpy as jnp
from jax import lax
from jax.experimental import pallas as pl
from jax.experimental.pallas import tpu as pltpu
from jax.sharding import PartitionSpec as P

MESH = pl.DeviceIdType.MESH
BF = jnp.bfloat16
F32 = jnp.float32
LANES = 128
AHEAD = 1
DIRECT = 1
LAG_SECOND = 3
LAG_FINAL = 5


def pair_list(fields):
    return [(i, j) for i in range(fields) for j in range(i + 1, fields)]


def kernel(
    size_gx, size_gy,
    pooled_hbm, cot_hbm, bil_hbm, bag_hbm, lens_hbm, home_hbm,
    out_ref, wout_ref,
    pooled_ref, cot_ref, bil_ref, bag_ref, lens_ref, home_ref,
    pool_f, proj_f,
    notes, gath, keep, part1, got1, part2, got2,
    w0, wsib, w1s, w1, w2, w3,
    ls, cs,
    ms, mr, zs, zr, ss, sr, p1s, p1r, p2s, p2r,
    was, war, w1ss, w1rs, w2ss, w2rs, w3ss, w3rs, wbs, wbr,
):
    samples, fields, width = pooled_ref.shape
    bag = bag_ref.shape[1]
    rows = keep.shape[2]
    nz, ny = size_gx // 2, size_gy // 2
    npc = 2 * ny
    gx, gy = lax.axis_index("gx"), lax.axis_index("gy")
    z, x, y, c = gx // 2, gx % 2, gy // 2, gy % 2
    spot = x * ny + y
    sibling = (gx, y * 2 + 1 - c)
    across = (z * 2 + 1 - x, gy)

    def spot_peer(d):
        to = (spot + d) % npc
        return (z * 2 + to // ny, (to % ny) * 2 + c)

    def row_peer(d):
        return (gx, ((y + d) % ny) * 2 + c)

    def z_peer(d):
        return (((z + d) % nz) * 2 + x, gy)

    def z_side(up, hop=1):
        return ((z + hop if up else z - hop) * 2 + x, gy)

    def z_reaches(up, hop=1):
        return z < nz - hop if up else z >= hop

    def remote(src, dst, send, recv, dev):
        return pltpu.make_async_remote_copy(
            src_ref=src, dst_ref=dst, send_sem=send, recv_sem=recv,
            device_id=dev, device_id_type=MESH,
        )

    def m_copy(s, up, hop=1):
        return remote(
            notes.at[0, s], notes.at[0, s], ms.at[int(up) + 2 * (hop - 1), s], mr.at[0, s],
            z_side(up, hop),
        )

    def ms_copy(s):
        return remote(notes.at[0, s], notes.at[1, s], ms.at[4, s], mr.at[1, s], sibling)

    def z_copy(f, s, up, hop=1):
        i = f * nz + s
        return remote(
            gath.at[f, 0, s], gath.at[f, 0, s], zs.at[int(up) + 2 * (hop - 1), i], zr.at[i],
            z_side(up, hop),
        )

    def s_copy(f, s):
        i = f * nz + s
        return remote(gath.at[f, 0, s], gath.at[f, 1, s], ss.at[i], sr.at[i], sibling)

    def first_copy(f, j, dev):
        return remote(part1.at[f, j], got1.at[f, j], p1s.at[f, j], p1r.at[f, j], dev)

    def second_copy(f, j, dev):
        return remote(part2.at[f, j], got2.at[f, j], p2s.at[f, j], p2r.at[f, j], dev)

    def wa_copy():
        return remote(w0.at[pl.ds((1 - c) * npc, npc)], wsib, was.at[0], war.at[0], sibling)

    def w1_copy(d):
        return remote(w1s.at[(spot + d) % npc], w1.at[d], w1ss.at[d], w1rs.at[d], spot_peer(d))

    def w2_copy(d, slot):
        return remote(w2.at[z], w2.at[slot], w2ss.at[d], w2rs.at[slot], z_peer(d))

    def w3_copy(d, slot):
        return remote(
            w3.at[c * npc + spot], w3.at[slot], w3ss.at[d], w3rs.at[d], spot_peer(d)
        )

    def wb_copy(half):
        at = pl.ds(half * npc, npc)
        return remote(w3.at[at], w3.at[at], wbs.at[0], wbr.at[0], sibling)

    pairs = pair_list(fields)
    number = {pair: p for p, pair in enumerate(pairs)}
    first = [number[i, i + 1] for i in range(fields - 1)]

    def cot_load(i):
        at = pl.ds(first[i], fields - 1 - i)
        return pltpu.make_async_copy(cot_hbm.at[at], cot_ref.at[at], cs.at[i])

    loads = [
        pltpu.make_async_copy(src, dst, ls.at[n])
        for n, (src, dst) in enumerate([
            (pooled_hbm, pooled_ref), (bil_hbm, bil_ref), (bag_hbm, bag_ref),
            (lens_hbm, lens_ref), (home_hbm, home_ref),
        ])
    ]
    loads[0].start()
    cot_load(0).start()
    for load in loads[1:]:
        load.start()
    for i in range(1, fields - 1):
        cot_load(i).start()

    barrier = pltpu.get_barrier_semaphore()
    for d in range(1, nz):
        pl.semaphore_signal(barrier, inc=1, device_id=z_peer(d), device_id_type=MESH)
    for d in range(1, npc):
        pl.semaphore_signal(barrier, inc=1, device_id=spot_peer(d), device_id_type=MESH)
    pl.semaphore_signal(barrier, inc=1, device_id=sibling, device_id_type=MESH)

    def spread_out(b, carry):
        pool_f[pl.ds(pl.multiple_of(b * fields, fields), fields), :] = pooled_ref[b].astype(F32)
        return carry

    def write_notes():
        for load in loads[2:]:
            load.wait()
        bags = [bag_ref[:, k, :] for k in range(bag)]
        high = [b // LANES for b in bags]
        low = [b % LANES for b in bags]

        def look(h, found):
            row = home_ref[:, pl.ds(pl.multiple_of(h * LANES, LANES), LANES)]
            return tuple(
                jnp.where(high[k] == h, jnp.take_along_axis(row, low[k], axis=1), found[k])
                for k in range(bag)
            )

        none = jnp.full(lens_ref.shape, 0, jnp.int32)
        found = lax.fori_loop(0, home_ref.shape[1] // LANES, look, (none,) * bag, unroll=8)
        lens = lens_ref[...]
        live = [jnp.where(lens > k, found[k], -1) for k in range(bag)]
        for k in range(bag):
            times = None
            for other in live:
                same = jnp.where(live[k] == other, 1, 0)
                times = same if times is None else times + same
            notes[0, z, :, k, :] = live[k] * 8 + jnp.where(live[k] < 0, 0, times)

    loads[0].wait()
    lax.fori_loop(0, samples, spread_out, 0, unroll=8)
    loads[1].wait()

    pool = lambda f: pool_f[pl.ds(f, samples, stride=fields), :]
    cot = lambda i, j: cot_ref[number[i, j]].astype(F32)
    piece = w0.shape[1]

    def send_own(copy):
        for hop in (2, 1):
            for up in (False, True):
                @pl.when(z_reaches(up, hop))
                def _():
                    copy(up, hop).start()

    for i in range(fields):
        total = None
        if i < fields - 1:
            cot_load(i).wait()
            mine = pool(i).astype(BF)
            upper = jnp.zeros((samples, width), F32)
            for j in range(i + 1, fields):
                upper = upper + cot(i, j) * pool(j)
            upper = upper.astype(BF)
            total = lax.dot_general(
                upper, bil_ref[i], (((1,), (1,)), ((), ())), preferred_element_type=F32
            )
        for k in range(i):
            term = cot(k, i) * proj_f[k]
            total = term if total is None else total + term
        gath[i, 0, z] = total.astype(BF)
        if i == 0:
            pl.semaphore_wait(barrier, nz - 1 + npc - 1 + 1)
        send_own(lambda up, hop: z_copy(i, z, up, hop))
        s_copy(i, z).start()
        if i == 0:
            write_notes()
            send_own(lambda up, hop: m_copy(z, up, hop))
            ms_copy(z).start()
        if i < fields - 1:
            proj_f[i] = jnp.dot(mine, bil_ref[i], preferred_element_type=F32)
            wide_w = lax.dot_general(
                mine, upper, (((0,), (0,)), ((), ())), preferred_element_type=F32
            )
            at, end = i * width, (i + 1) * width
            while at < end:
                p, r = at // piece, at % piece
                n = min(piece - r, end - at)
                w0[p, r : r + n, :] = wide_w[at - i * width : at - i * width + n, :]
                at += n

    wa_copy().start()

    def take(arrived, onward, to_sibling):
        for o in range(1, nz):
            for up in (True, False):
                s = z - o if up else z + o

                @pl.when(s >= 0 if up else s < nz)
                def _():
                    arrived(s)

                    if o > 1:
                        @pl.when(z_reaches(up))
                        def _():
                            onward(s, up)

                    to_sibling(s)

    def receive(f):
        take(
            lambda s: z_copy(f, s, True).wait_recv(),
            lambda s, up: z_copy(f, s, up).start(),
            lambda s: s_copy(f, s).start(),
        )

    take(
        lambda s: m_copy(s, True).wait_recv(),
        lambda s, up: m_copy(s, up).start(),
        lambda s: ms_copy(s).start(),
    )

    for s in range(nz):
        ms_copy(s).wait_recv()

    row_number = lax.broadcasted_iota(jnp.int32, (rows, samples), 0).astype(F32).astype(BF)
    zero = jnp.zeros((), BF)

    def sums_for(f, x_to, y_to):
        base = ((z * 2 + x_to) * size_gy + y_to * 2 + c) * rows
        blocks, values = [], []
        for core in range(2):
            for s in range(nz):
                note = notes[core, s, f]
                key = ((note >> 3) - base).astype(F32).astype(BF)
                times = (note & 7).astype(F32).astype(BF)
                count = zero
                for k in range(bag):
                    count = jnp.where(
                        row_number == key[k : k + 1, :], times[k : k + 1, :], count
                    )
                blocks.append(count)
                values.append(gath[f, core, s])
        return jnp.dot(
            jnp.concatenate(blocks, axis=1),
            jnp.concatenate(values, axis=0),
            preferred_element_type=F32,
        )

    def by_x(f):
        return jnp.logical_and(f % 2 == 0, f < fields - DIRECT)

    def by_y(f):
        return jnp.logical_and(f % 2 == 1, f < fields - DIRECT)

    def straight(f):
        return f >= fields - DIRECT

    def field_sums(f):
        for s in range(nz):
            s_copy(f, s).wait_recv()

        def one_target(j, carry):
            d_x = jnp.where(j < ny, j, j - ny + 1)
            d_y = jnp.where(j == npc - 2, 0, jnp.where(j < ny - 1, j + 1, j - ny + 2))
            other_x, other_y = j < ny, jnp.logical_or(j < ny - 1, j == npc - 2)
            d = jnp.where(by_x(f), d_x, d_y)
            x_to = jnp.where(jnp.where(by_x(f), other_x, other_y), 1 - x, x)
            y_to = (y + d) % ny
            to = (spot + npc - 1 - j) % npc
            x_to = jnp.where(straight(f), to // ny, x_to)
            y_to = jnp.where(straight(f), to % ny, y_to)
            mine = j == npc - 1
            total = sums_for(f, jnp.where(mine, x, x_to), jnp.where(mine, y, y_to))
            sent = jnp.where(by_x(f), j < ny, jnp.where(by_y(f), j < npc - 2, j < npc - 1))

            @pl.when(sent)
            def _():
                part1[f, j] = total.astype(BF)

                @pl.when(by_x(f))
                def _():
                    first_copy(f, j, across).start()

                @pl.when(by_y(f))
                def _():
                    first_copy(f, j, row_peer(d)).start()

                @pl.when(straight(f))
                def _():
                    first_copy(f, j, spot_peer(npc - 1 - j)).start()

            @pl.when(jnp.logical_and(by_x(f), jnp.logical_and(j >= ny, j < npc - 1)))
            def _():
                keep[f, j - ny] = total

            @pl.when(jnp.logical_and(by_y(f), j == npc - 2))
            def _():
                keep[f, 0] = total

            @pl.when(mine)
            def _():
                out_ref[pl.ds(f, rows, stride=fields), :] = total

            return carry

        lax.fori_loop(0, npc, one_target, 0)

    def second_step(f):
        @pl.when(by_x(f))
        def _():
            for j in range(ny):
                first_copy(f, j, across).wait_recv()
            for d in range(1, ny):
                part2[f, d - 1] = (keep[f, d - 1] + got1[f, d].astype(F32)).astype(BF)
                second_copy(f, d - 1, row_peer(d)).start()

        @pl.when(by_y(f))
        def _():
            for j in range(npc - 2):
                first_copy(f, j, sibling).wait_recv()
            total = keep[f, 0]
            for j in range(ny - 1):
                total = total + got1[f, j].astype(F32)
            part2[f, 0] = total.astype(BF)
            second_copy(f, 0, across).start()

    def last_step(f):
        at = pl.ds(f, rows, stride=fields)

        @pl.when(by_x(f))
        def _():
            total = out_ref[at, :] + got1[f, 0].astype(F32)
            for j in range(ny - 1):
                second_copy(f, j, sibling).wait_recv()
                total = total + got2[f, j].astype(F32)
            out_ref[at, :] = total

        @pl.when(by_y(f))
        def _():
            total = out_ref[at, :]
            for j in range(ny - 1, npc - 2):
                total = total + got1[f, j].astype(F32)
            second_copy(f, 0, sibling).wait_recv()
            out_ref[at, :] = total + got2[f, 0].astype(F32)

        @pl.when(straight(f))
        def _():
            total = out_ref[at, :]
            for j in range(npc - 1):
                first_copy(f, j, sibling).wait_recv()
                total = total + got1[f, j].astype(F32)
            out_ref[at, :] = total

    def weights_in_plane():
        wa_copy().wait_recv()
        for d in range(1, npc):
            to = (spot + d) % npc
            w1s[to] = (w0[c * npc + to] + wsib[to]).astype(BF)
            w1_copy(d).start()

    def weights_along_z():
        total = w0[c * npc + spot] + wsib[spot]
        for d in range(1, npc):
            w1_copy(d).wait_recv()
            total = total + w1[d].astype(F32)
        w2[z] = total.astype(BF)
        for d in range(1, nz):
            w2_copy(d, z).start()

    def weights_back():
        for d in range(1, nz):
            w2_copy(d, (z + d) % nz).wait_recv()
        total = w2[0].astype(F32)
        for s in range(1, nz):
            total = total + w2[s].astype(F32)
        w3[c * npc + spot] = total.astype(BF)
        for d in range(1, npc):
            w3_copy(d, c * npc + spot).start()

    def weights_to_sibling():
        for d in range(1, npc):
            w3_copy(d, c * npc + (spot - d) % npc).wait_recv()
        wb_copy(c).start()

    for f in range(min(fields, AHEAD)):
        receive(f)

    def one_field(f, carry):
        @pl.when(f + AHEAD < fields)
        def _():
            receive(f + AHEAD)

        field_sums(f)

        for at, step in (
            (0, weights_in_plane), (2, weights_along_z),
            (4, weights_back), (6, weights_to_sibling),
        ):
            @pl.when(f == at)
            def _():
                step()

        @pl.when(f >= LAG_SECOND)
        def _():
            second_step(f - LAG_SECOND)

        @pl.when(f >= LAG_FINAL)
        def _():
            last_step(f - LAG_FINAL)

        return carry

    lax.fori_loop(0, fields, one_field, 0)

    def late_second(f, carry):
        second_step(f)
        return carry

    lax.fori_loop(fields - LAG_SECOND, fields, late_second, 0)
    wb_copy(1 - c).wait_recv()
    wout_ref[...] = w3[...].astype(F32)

    def late_last(f, carry):
        last_step(f)
        return carry

    lax.fori_loop(fields - LAG_FINAL, fields, late_last, 0)

    def drain_z(sent):
        for up in (False, True):
            for hop in (1, 2):
                @pl.when(z_reaches(up, hop))
                def _():
                    sent(z, up, hop).wait_send()
            for o in range(2, nz - 1):
                s = z - o if up else z + o

                @pl.when(jnp.logical_and(z_reaches(up), s >= 0 if up else s < nz))
                def _():
                    sent(s, up, 1).wait_send()

    drain_z(m_copy)
    for s in range(nz):
        ms_copy(s).wait_send()

    def drain(f, carry):
        drain_z(lambda s, up, hop: z_copy(f, s, up, hop))
        for s in range(nz):
            s_copy(f, s).wait_send()

        @pl.when(by_x(f))
        def _():
            for j in range(ny):
                first_copy(f, j, across).wait_send()
            for j in range(ny - 1):
                second_copy(f, j, across).wait_send()

        @pl.when(by_y(f))
        def _():
            for j in range(npc - 2):
                first_copy(f, j, across).wait_send()
            second_copy(f, 0, across).wait_send()

        @pl.when(straight(f))
        def _():
            for j in range(npc - 1):
                first_copy(f, j, across).wait_send()

        return carry

    lax.fori_loop(0, fields, drain, 0)
    wa_copy().wait_send()
    wb_copy(c).wait_send()
    for d in range(1, nz):
        w2_copy(d, z).wait_send()
    for d in range(1, npc):
        w1_copy(d).wait_send()
        w3_copy(d, c * npc + spot).wait_send()


def on_device(size_gx, size_gy, pooled, cotangent, bilinear, bag_ids, bag_lens, row_home):
    samples, fields, width = pooled.shape
    bag = bag_ids.shape[2]
    rows = row_home.shape[1] // (size_gx * size_gy)
    nz, ny, plane = size_gx // 2, size_gy // 2, 2 * size_gy
    npc = 2 * ny
    pairs = fields * (fields - 1) // 2
    piece = (fields - 1) * width // plane
    nb1, nb2 = npc - 1, ny - 1
    vmem = pl.BlockSpec(memory_space=pltpu.VMEM)
    hbm = pl.BlockSpec(memory_space=pltpu.HBM)
    dma = pltpu.SemaphoreType.DMA
    buffers = [
        ((samples, fields, width), BF),
        ((pairs, samples, width), BF),
        ((fields - 1, width, width), BF),
        ((fields, bag, samples), jnp.int32),
        ((fields, samples), jnp.int32),
        (row_home.shape, jnp.int32),
        ((samples * fields, width), F32),
        ((fields - 1, samples, width), F32),
        ((2, nz, fields, bag, samples), jnp.int32),
        ((fields, 2, nz, samples, width), BF),
        ((fields, nb2, rows, width), F32),
        ((fields, nb1, rows, width), BF),
        ((fields, nb1, rows, width), BF),
        ((fields, nb2, rows, width), BF),
        ((fields, nb2, rows, width), BF),
        ((plane, piece, width), F32),
        ((npc, piece, width), F32),
        ((npc, piece, width), BF),
        ((npc, piece, width), BF),
        ((nz, piece, width), BF),
        ((plane, piece, width), BF),
    ]
    held = sum(math.prod(shape) * jnp.dtype(kind).itemsize for shape, kind in buffers)
    table, weight = pl.pallas_call(
        functools.partial(kernel, size_gx, size_gy),
        out_shape=(
            jax.ShapeDtypeStruct((rows * fields, width), F32),
            jax.ShapeDtypeStruct((plane, piece, width), F32),
        ),
        in_specs=[hbm] * 6,
        out_specs=(vmem,) * 2,
        scratch_shapes=[pltpu.VMEM(shape, kind) for shape, kind in buffers] + [
            dma((5,)),
            dma((fields - 1,)),
            dma((5, nz)),
            dma((2, nz)),
            dma((4, fields * nz)),
            dma((fields * nz,)),
            dma((fields * nz,)),
            dma((fields * nz,)),
            dma((fields, nb1)),
            dma((fields, nb1)),
            dma((fields, nb2)),
            dma((fields, nb2)),
            dma((1,)),
            dma((1,)),
            dma((npc,)),
            dma((npc,)),
            dma((nz,)),
            dma((nz,)),
            dma((npc,)),
            dma((npc,)),
            dma((1,)),
            dma((1,)),
        ],
        compiler_params=pltpu.CompilerParams(
            collective_id=0, has_side_effects=True, vmem_limit_bytes=held + (10 << 20)
        ),
    )(*(pltpu.with_memory_space_constraint(v, pltpu.HBM) for v in (
        pooled, cotangent.transpose(1, 0, 2), bilinear,
        bag_ids.transpose(1, 2, 0), bag_lens.transpose(1, 0), row_home,
    )))
    return (
        weight.reshape(fields - 1, width, width),
        table.reshape(rows, fields, width),
    )


def solution(mesh):
    placed = (
        P(("gx", "gy"), None, None),
        P(("gx", "gy"), None, None),
        P(),
        P(("gx", "gy"), None, None),
        P(("gx", "gy"), None),
        P(),
    )
    return jax.shard_map(
        functools.partial(on_device, mesh.shape["gx"], mesh.shape["gy"]),
        mesh=mesh,
        in_specs=placed,
        out_specs=(P(), P(("gx", "gy"), None, None)),
        check_vma=False,
    )
```

```python
import functools
import math

import jax
import jax.numpy as jnp
from jax import lax
from jax.experimental import pallas as pl
from jax.experimental.pallas import tpu as pltpu
from jax.sharding import PartitionSpec as P

MESH = pl.DeviceIdType.MESH
BF = jnp.bfloat16
F32 = jnp.float32
LANES = 128
GROUP = 4
EARLY = 2
W1 = -2
W2 = 0
W3 = 3
W4 = 5
W5 = 7
AHEAD_END = 1
AHEAD_MID = 2
DIRECT = 1
LAG_SECOND = 3
LAG_FINAL = 5


def pair_list(fields):
    return [(i, j) for i in range(fields) for j in range(i + 1, fields)]


def kernel(
    size_gx, size_gy,
    pooled_hbm, cot_hbm, bil_hbm, bag_hbm, lens_hbm, home_hbm,
    out_ref, wout_ref,
    pooled_ref, cot_ref, bil_ref, bag_ref, lens_ref, home_ref,
    pool_f, proj_f, upper_b,
    notes, gath, sums, keep, part1, got1, part2, got2,
    w0, wsib, w1s, w1, w2f, w2s, w2, wz, w3,
    ls, cs,
    ms, mr, zs, zr, ss, sr, p1s, p1r, p2s, p2r,
    was, war, w1ss, w1rs, w2ss, w2rs, wzss, wzrs, w3ss, w3rs, wbs, wbr,
):
    samples, fields, width = pooled_ref.shape
    bag = bag_ref.shape[1]
    rows = keep.shape[2]
    part1_of, part2_of = part1.shape[0] // fields, part2.shape[0] // fields
    nz, ny = size_gx // 2, size_gy // 2
    npc = 2 * ny
    gx, gy = lax.axis_index("gx"), lax.axis_index("gy")
    z, x, y, c = gx // 2, gx % 2, gy // 2, gy % 2
    spot = x * ny + y
    sibling = (gx, y * 2 + 1 - c)
    across = (z * 2 + 1 - x, gy)

    def spot_peer(d):
        to = (spot + d) % npc
        return (z * 2 + to // ny, (to % ny) * 2 + c)

    def row_peer(d):
        return (gx, ((y + d) % ny) * 2 + c)

    def far_peer(d):
        return (z * 2 + 1 - x, ((y + d) % ny) * 2 + c)

    def z_peer(d):
        return (((z + d) % nz) * 2 + x, gy)

    def z_side(up, hop=1):
        return ((z + hop if up else z - hop) * 2 + x, gy)

    def z_reaches(up, hop=1):
        return z < nz - hop if up else z >= hop

    def z_forwards(up):
        return jnp.logical_and(z_reaches(up), z >= 2 if up else z < nz - 2)

    def remote(src, dst, send, recv, dev):
        return pltpu.make_async_remote_copy(
            src_ref=src, dst_ref=dst, send_sem=send, recv_sem=recv,
            device_id=dev, device_id_type=MESH,
        )

    def m_copy(d, slot):
        return remote(notes.at[0, z], notes.at[0, slot], ms.at[0], mr.at[slot], z_peer(d))

    def ms_copy(s):
        return remote(notes.at[0, s], notes.at[1, s], ms.at[1], mr.at[nz], sibling)

    def z_copy(f, s, up, hop=1):
        kind = 0 if hop == 2 else 1 + jnp.where(s == z, 0, 1)
        return remote(
            gath.at[f, 0, s], gath.at[f, 0, s], zs.at[int(up), kind], zr.at[f * nz + s],
            z_side(up, hop),
        )

    def s_copy(f, s):
        return remote(gath.at[f, 0, s], gath.at[f, 1, s], ss.at[0], sr.at[f], sibling)

    def s_copies(f):
        return remote(gath.at[f, 0], gath.at[f, 1], ss.at[0], sr.at[f], sibling)

    def first_copy(f, j, dev):
        at = f * part1_of + j
        return remote(part1.at[at], got1.at[at], p1s.at[0], p1r.at[at], dev)

    def second_copy(f, j, dev):
        at = f * part2_of + j
        return remote(part2.at[at], got2.at[at], p2s.at[0], p2r.at[at], dev)

    def wa_copy():
        return remote(w0.at[pl.ds((1 - c) * npc, npc)], wsib, was.at[0], war.at[0], sibling)

    def w1_copy(d):
        return remote(w1s.at[(spot + d) % npc], w1.at[d], w1ss.at[d], w1rs.at[d], spot_peer(d))

    def w2_copy(d):
        return remote(w2s.at[(z + d) % nz], w2.at[d], w2ss.at[d], w2rs.at[d], z_peer(d))

    def wz_copy(d, slot):
        return remote(wz.at[z], wz.at[slot], wzss.at[d], wzrs.at[d], z_peer(d))

    def w3_copy(d, slot):
        return remote(
            w3.at[c * npc + spot], w3.at[slot], w3ss.at[d], w3rs.at[d], spot_peer(d)
        )

    def wb_copy(half):
        at = pl.ds(half * npc, npc)
        return remote(w3.at[at], w3.at[at], wbs.at[0], wbr.at[0], sibling)

    pairs = pair_list(fields)
    number = {pair: p for p, pair in enumerate(pairs)}
    first = [number[i, i + 1] for i in range(fields - 1)]

    def cot_load(i):
        at = pl.ds(first[i], fields - 1 - i)
        return pltpu.make_async_copy(cot_hbm.at[at], cot_ref.at[at], cs.at[i])

    loads = [
        pltpu.make_async_copy(src, dst, ls.at[n])
        for n, (src, dst) in enumerate([
            (pooled_hbm, pooled_ref), (bil_hbm, bil_ref), (bag_hbm, bag_ref),
            (lens_hbm, lens_ref), (home_hbm, home_ref),
        ])
    ]
    for n in (4, 2, 3, 0):
        loads[n].start()
    cot_load(0).start()
    loads[1].start()
    for i in range(1, fields - 1):
        cot_load(i).start()

    barrier = pltpu.get_barrier_semaphore()
    for d in range(1, nz):
        pl.semaphore_signal(barrier, inc=1, device_id=z_peer(d), device_id_type=MESH)
    for d in range(1, npc):
        pl.semaphore_signal(barrier, inc=1, device_id=spot_peer(d), device_id_type=MESH)
    pl.semaphore_signal(barrier, inc=1, device_id=sibling, device_id_type=MESH)

    def spread_out(b, carry):
        pool_f[pl.ds(pl.multiple_of(b * fields, fields), fields), :] = pooled_ref[b].astype(F32)
        return carry

    def write_notes():
        for load in loads[2:]:
            load.wait()
        bags = [bag_ref[:, k, :] for k in range(bag)]
        high = [b // LANES for b in bags]
        low = [b % LANES for b in bags]

        def look(h, found):
            row = home_ref[:, pl.ds(pl.multiple_of(h * LANES, LANES), LANES)]
            return tuple(
                jnp.where(high[k] == h, jnp.take_along_axis(row, low[k], axis=1), found[k])
                for k in range(bag)
            )

        none = jnp.full(lens_ref.shape, 0, jnp.int32)
        found = lax.fori_loop(0, home_ref.shape[1] // LANES, look, (none,) * bag, unroll=64)
        lens = lens_ref[...]
        live = [jnp.where(lens > k, found[k], -1) for k in range(bag)]
        for k in range(bag):
            times = None
            for other in live:
                same = jnp.where(live[k] == other, 1, 0)
                times = same if times is None else times + same
            notes[0, z, :, k, :] = live[k] * 8 + jnp.where(live[k] < 0, 0, times)

    write_notes()
    loads[0].wait()
    lax.fori_loop(0, samples, spread_out, 0, unroll=8)
    loads[1].wait()

    pool = lambda f: pool_f[pl.ds(f, samples, stride=fields), :]
    cot = lambda i, j: cot_ref[number[i, j]].astype(F32)
    piece, share = w0.shape[1], wz.shape[1]

    def send_own(copy, early=True):
        for hop in (2, 1):
            for up in (False, True):
                ok = z_reaches(up, hop)
                if hop == 1 and not early:
                    ok = jnp.logical_and(ok, jnp.logical_not(z_forwards(up)))

                @pl.when(ok)
                def _():
                    copy(up, hop).start()

    for i in range(fields):
        total = None
        if i < fields - 1:
            cot_load(i).wait()
            mine = pool(i).astype(BF)
            upper = jnp.zeros((samples, width), F32)
            for j in range(i + 1, fields):
                upper = upper + cot(i, j) * pool(j)
            upper = upper.astype(BF)
            total = lax.dot_general(
                upper, bil_ref[i], (((1,), (1,)), ((), ())), preferred_element_type=F32
            )
        for k in range(i):
            term = cot(k, i) * proj_f[k]
            total = term if total is None else total + term
        gath[i, 0, z] = total.astype(BF)
        if i == 0:
            pl.semaphore_wait(barrier, nz - 1 + npc - 1 + 1)
            for d in range(1, nz):
                m_copy(d, z).start()
            ms_copy(z).start()
        send_own(lambda up, hop: z_copy(i, z, up, hop), i < EARLY)
        s_copy(i, z).start()
        if i < fields - 1:
            upper_b[i] = upper
            proj_f[i] = jnp.dot(mine, bil_ref[i], preferred_element_type=F32)

    def weights_here():
        for i in range(fields - 1):
            wide_w = lax.dot_general(
                pool(i).astype(BF), upper_b[i], (((0,), (0,)), ((), ())),
                preferred_element_type=F32,
            )
            at, end = i * width, (i + 1) * width
            while at < end:
                p, r = at // piece, at % piece
                n = min(piece - r, end - at)
                w0[p, r : r + n, :] = wide_w[at - i * width : at - i * width + n, :]
                at += n
        wa_copy().start()

    weights_here()

    def take(arrived, onward, to_sibling):
        for o in range(1, nz):
            for up in (True, False):
                s = z - o if up else z + o

                @pl.when(s >= 0 if up else s < nz)
                def _():
                    arrived(s)

                    if o > 1:
                        @pl.when(z_reaches(up))
                        def _():
                            onward(s, up)

                    to_sibling(s)

    def receive(f):
        take(
            lambda s: z_copy(f, s, True).wait_recv(),
            lambda s, up: z_copy(f, s, up).start(),
            lambda s: s_copy(f, s).start(),
        )
        for up in (False, True):
            @pl.when(jnp.logical_and(z_forwards(up), f + EARLY < fields))
            def _():
                z_copy(f + EARLY, z, up).start()

    for d in range(1, nz):
        s = (z + d) % nz
        m_copy(d, s).wait_recv()
        ms_copy(s).start()

    steps = (
        (W1, lambda: weights_in_plane()), (W2, lambda: weights_along_z()),
        (W3, lambda: weights_back_z()), (W4, lambda: weights_back()),
        (W5, lambda: weights_to_sibling()),
    )

    row_number = lax.broadcasted_iota(jnp.int32, (rows, samples), 0).astype(F32).astype(BF)
    zero = jnp.zeros((), BF)

    def owner_of(t):
        return 1 - x if t // ny == 1 else x, (y + t % ny) % ny

    def add_half(f, core):
        fresh = core == 0
        for t0 in range(0, npc, GROUP):
            totals = [None] * GROUP
            for s in range(0, nz, 2):
                held = jnp.concatenate([gath[f, core, s], gath[f, core, s + 1]], axis=0)
                place = [notes[core, s + e, f] >> 3 for e in range(2)]
                times = [(notes[core, s + e, f] & 7).astype(F32).astype(BF) for e in range(2)]
                for t in range(GROUP):
                    x_to, y_to = owner_of(t0 + t)
                    base = ((z * 2 + x_to) * size_gy + y_to * 2 + c) * rows
                    blocks = []
                    for e in range(2):
                        key = (place[e] - base).astype(F32).astype(BF)
                        count = zero
                        for k in range(bag):
                            count = jnp.where(
                                row_number == key[k : k + 1, :], times[e][k : k + 1, :], count
                            )
                        blocks.append(count)
                    part = jnp.dot(
                        jnp.concatenate(blocks, axis=1), held, preferred_element_type=F32
                    )
                    totals[t] = part if totals[t] is None else totals[t] + part
            for t in range(GROUP):
                sums[t0 + t] = totals[t] if fresh else sums[t0 + t] + totals[t]

    def by_x(f):
        return jnp.logical_and(f % 2 == 0, f < fields - DIRECT)

    def by_y(f):
        return jnp.logical_and(f % 2 == 1, f < fields - DIRECT)

    def straight(f):
        return f >= fields - DIRECT

    def field_sums(f):
        add_half(f, 0)
        s_copies(f).wait_recv()
        add_half(f, 1)

        @pl.when(by_x(f))
        def _():
            for d in range(ny):
                part1[f * part1_of + d] = sums[ny + d].astype(BF)
                first_copy(f, d, across).start()
            for d in range(1, ny):
                keep[f, d - 1] = sums[d]

        @pl.when(by_y(f))
        def _():
            for d in range(1, ny):
                part1[f * part1_of + d - 1] = sums[ny + d].astype(BF)
                first_copy(f, d - 1, row_peer(d)).start()
                part1[f * part1_of + ny + d - 2] = sums[d].astype(BF)
                first_copy(f, ny + d - 2, row_peer(d)).start()
            keep[f, 0] = sums[ny]

        @pl.when(straight(f))
        def _():
            for d in range(ny - 1, -1, -1):
                for other in (1, 0):
                    t = other * ny + d
                    if t:
                        part1[f * part1_of + t - 1] = sums[t].astype(BF)
                        dev = across if d == 0 else row_peer(d) if other == 0 else far_peer(d)
                        first_copy(f, t - 1, dev).start()

        out_ref[pl.ds(f, rows, stride=fields), :] = sums[0]

    def second_step(f):
        @pl.when(by_x(f))
        def _():
            for j in range(ny):
                first_copy(f, j, across).wait_recv()
            for d in range(1, ny):
                part2[f * part2_of + d - 1] = (keep[f, d - 1] + got1[f * part1_of + d].astype(F32)).astype(BF)
                second_copy(f, d - 1, row_peer(d)).start()

        @pl.when(by_y(f))
        def _():
            for j in range(npc - 2):
                first_copy(f, j, sibling).wait_recv()
            total = keep[f, 0]
            for j in range(ny - 1):
                total = total + got1[f * part1_of + j].astype(F32)
            part2[f * part2_of + 0] = total.astype(BF)
            second_copy(f, 0, across).start()

    def last_step(f):
        at = pl.ds(f, rows, stride=fields)

        @pl.when(by_x(f))
        def _():
            total = out_ref[at, :] + got1[f * part1_of + 0].astype(F32)
            for j in range(ny - 1):
                second_copy(f, j, sibling).wait_recv()
                total = total + got2[f * part2_of + j].astype(F32)
            out_ref[at, :] = total

        @pl.when(by_y(f))
        def _():
            total = out_ref[at, :]
            for j in range(ny - 1, npc - 2):
                total = total + got1[f * part1_of + j].astype(F32)
            second_copy(f, 0, sibling).wait_recv()
            out_ref[at, :] = total + got2[f * part2_of + 0].astype(F32)

        @pl.when(straight(f))
        def _():
            total = out_ref[at, :]
            for j in range(npc - 1):
                first_copy(f, j, sibling).wait_recv()
                total = total + got1[f * part1_of + j].astype(F32)
            out_ref[at, :] = total

    def weights_in_plane():
        wa_copy().wait_recv()
        for d in range(1, npc):
            to = (spot + d) % npc
            w1s[to] = (w0[c * npc + to] + wsib[to]).astype(BF)
            w1_copy(d).start()

    def slices(r):
        return slice(min(piece, r * share), min(piece, (r + 1) * share))

    def weights_along_z():
        total = w0[c * npc + spot] + wsib[spot]
        for d in range(1, npc):
            w1_copy(d).wait_recv()
            total = total + w1[d].astype(F32)
        for r in range(-(-piece // share)):
            rows_r = total[slices(r)]
            w2f[r, : rows_r.shape[0]] = rows_r
            w2s[r, : rows_r.shape[0]] = rows_r.astype(BF)
        for d in range(1, nz):
            w2_copy(d).start()

    def weights_back_z():
        total = w2f[z]
        for d in range(1, nz):
            w2_copy(d).wait_recv()
            total = total + w2[d].astype(F32)
        wz[z] = total.astype(BF)
        for d in range(1, nz):
            wz_copy(d, z).start()

    def weights_back():
        for d in range(1, nz):
            wz_copy(d, (z - d) % nz).wait_recv()
        for r in range(-(-piece // share)):
            at = slices(r)
            w3[c * npc + spot, at] = wz[r, : at.stop - at.start]
        for d in range(1, npc):
            w3_copy(d, c * npc + spot).start()

    def weights_to_sibling():
        for d in range(1, npc):
            w3_copy(d, c * npc + (spot - d) % npc).wait_recv()
        wb_copy(c).start()

    def early_steps(n):
        for at, step in steps:
            if at == n:
                step()

    early_steps(-2)
    ahead = jnp.where(jnp.logical_and(z > 0, z < nz - 1), AHEAD_MID, AHEAD_END)
    for f in range(min(fields, max(AHEAD_MID, AHEAD_END))):
        @pl.when(f < ahead)
        def _():
            receive(f)

    early_steps(-1)
    remote(notes.at[0], notes.at[1], ms.at[1], mr.at[nz], sibling).wait_recv()

    def one_field(f, carry):
        @pl.when(f + ahead < fields)
        def _():
            receive(f + ahead)

        field_sums(f)

        for at, step in steps:
            if at >= 0:
                @pl.when(f == at)
                def _():
                    step()

        @pl.when(f >= LAG_SECOND)
        def _():
            second_step(f - LAG_SECOND)

        @pl.when(f >= LAG_FINAL)
        def _():
            last_step(f - LAG_FINAL)

        return carry

    lax.fori_loop(0, fields, one_field, 0)

    def late_second(f, carry):
        second_step(f)
        return carry

    lax.fori_loop(fields - LAG_SECOND, fields, late_second, 0)
    wb_copy(1 - c).wait_recv()
    wout_ref[...] = w3[...].astype(F32)

    def late_last(f, carry):
        last_step(f)
        return carry

    lax.fori_loop(fields - LAG_FINAL, fields, late_last, 0)

    def sent(ref, sem):
        remote(ref, ref, sem, zr.at[0], sibling).wait_send()

    for up in (False, True):
        for hop in (1, 2):
            @pl.when(z_reaches(up, hop))
            def _():
                sent(gath.at[:, 0, 0], zs.at[int(up), 2 - hop])
        for o in range(2, nz - 1):
            @pl.when(jnp.logical_and(z_reaches(up), z >= o if up else z < nz - o))
            def _():
                sent(gath.at[:, 0, 0], zs.at[int(up), 2])
    for d in range(1, nz):
        m_copy(d, z).wait_send()
    sent(notes.at[0], ms.at[1])
    sent(gath.at[:, 0], ss.at[0])
    two_step = range(fields - DIRECT)
    n1 = sum(ny if f % 2 == 0 else npc - 2 for f in two_step) + DIRECT * (npc - 1)
    n2 = sum(ny - 1 if f % 2 == 0 else 1 for f in two_step)
    sent(part1.at[pl.ds(0, n1)], p1s.at[0])
    sent(part2.at[pl.ds(0, n2)], p2s.at[0])
    wa_copy().wait_send()
    wb_copy(c).wait_send()
    for d in range(1, nz):
        w2_copy(d).wait_send()
        wz_copy(d, z).wait_send()
    for d in range(1, npc):
        w1_copy(d).wait_send()
        w3_copy(d, c * npc + spot).wait_send()


def on_device(size_gx, size_gy, pooled, cotangent, bilinear, bag_ids, bag_lens, row_home):
    samples, fields, width = pooled.shape
    bag = bag_ids.shape[2]
    rows = row_home.shape[1] // (size_gx * size_gy)
    nz, ny, plane = size_gx // 2, size_gy // 2, 2 * size_gy
    npc = 2 * ny
    pairs = fields * (fields - 1) // 2
    piece = (fields - 1) * width // plane
    nb1, nb2 = npc - 1, ny - 1
    share = -(-piece // nz)
    vmem = pl.BlockSpec(memory_space=pltpu.VMEM)
    hbm = pl.BlockSpec(memory_space=pltpu.HBM)
    dma = pltpu.SemaphoreType.DMA
    buffers = [
        ((samples, fields, width), BF),
        ((pairs, samples, width), BF),
        ((fields - 1, width, width), BF),
        ((fields, bag, samples), jnp.int32),
        ((fields, samples), jnp.int32),
        (row_home.shape, jnp.int32),
        ((samples * fields, width), F32),
        ((fields - 1, samples, width), F32),
        ((fields - 1, samples, width), BF),
        ((2, nz, fields, bag, samples), jnp.int32),
        ((fields, 2, nz, samples, width), BF),
        ((npc, rows, width), F32),
        ((fields, nb2, rows, width), F32),
        ((fields * nb1, rows, width), BF),
        ((fields * nb1, rows, width), BF),
        ((fields * nb2, rows, width), BF),
        ((fields * nb2, rows, width), BF),
        ((plane, piece, width), F32),
        ((npc, piece, width), F32),
        ((npc, piece, width), BF),
        ((npc, piece, width), BF),
        ((nz, share, width), F32),
        ((nz, share, width), BF),
        ((nz, share, width), BF),
        ((nz, share, width), BF),
        ((plane, piece, width), BF),
    ]
    held = sum(math.prod(shape) * jnp.dtype(kind).itemsize for shape, kind in buffers)
    table, weight = pl.pallas_call(
        functools.partial(kernel, size_gx, size_gy),
        out_shape=(
            jax.ShapeDtypeStruct((rows * fields, width), F32),
            jax.ShapeDtypeStruct((plane, piece, width), F32),
        ),
        in_specs=[hbm] * 6,
        out_specs=(vmem,) * 2,
        scratch_shapes=[pltpu.VMEM(shape, kind) for shape, kind in buffers] + [
            dma((5,)),
            dma((fields - 1,)),
            dma((2,)),
            dma((nz + 1,)),
            dma((2, 3)),
            dma((fields * nz,)),
            dma((1,)),
            dma((fields,)),
            dma((1,)),
            dma((fields * nb1,)),
            dma((1,)),
            dma((fields * nb2,)),
            dma((1,)),
            dma((1,)),
            dma((npc,)),
            dma((npc,)),
            dma((nz,)),
            dma((nz,)),
            dma((nz,)),
            dma((nz,)),
            dma((npc,)),
            dma((npc,)),
            dma((1,)),
            dma((1,)),
        ],
        compiler_params=pltpu.CompilerParams(
            collective_id=0, has_side_effects=True, vmem_limit_bytes=held + (10 << 20)
        ),
    )(*(pltpu.with_memory_space_constraint(v, pltpu.HBM) for v in (
        pooled, cotangent.transpose(1, 0, 2), bilinear,
        bag_ids.transpose(1, 2, 0), bag_lens.transpose(1, 0), row_home,
    )))
    return (
        weight.reshape(fields - 1, width, width),
        table.reshape(rows, fields, width),
    )


def solution(mesh):
    placed = (
        P(("gx", "gy"), None, None),
        P(("gx", "gy"), None, None),
        P(),
        P(("gx", "gy"), None, None),
        P(("gx", "gy"), None),
        P(),
    )
    return jax.shard_map(
        functools.partial(on_device, mesh.shape["gx"], mesh.shape["gy"]),
        mesh=mesh,
        in_specs=placed,
        out_specs=(P(), P(("gx", "gy"), None, None)),
        check_vma=False,
    )
```

```python
import functools
import math

import jax
import jax.numpy as jnp
from jax import lax
from jax.experimental import pallas as pl
from jax.experimental.pallas import tpu as pltpu
from jax.sharding import PartitionSpec as P

MESH = pl.DeviceIdType.MESH
BF = jnp.bfloat16
F32 = jnp.float32
LANES = 128
PLANE = 1
PLANE_AT = 6
GROUP = 4
EARLY = 2
W1 = -2
W2 = 1
W3 = 3
W4 = 5
W5 = 7
AHEAD_END = 0
AHEAD_MID = 2
DIRECT = 1
LAG_SECOND = 2
LAG_FINAL = 8


def pair_list(fields):
    return [(i, j) for i in range(fields) for j in range(i + 1, fields)]


def kernel(
    size_gx, size_gy,
    pooled_hbm, cot_hbm, bil_hbm, bag_hbm, lens_hbm, home_hbm,
    out_ref, wout_ref,
    pooled_ref, cot_ref, bil_ref, bag_ref, lens_ref, home_ref,
    pool_f, proj_f, upper_b,
    notes, notes_p, gath, gath_p, part_z, got_z, sums, keep, part1, got1, part2, got2,
    w0, wsib, w1s, w1, w2f, w2s, w2, wz, w3,
    ls, cs,
    ms, mr, ns, nr, gs, gr, hs, hr, zs, zr, ss, sr, p1s, p1r, p2s, p2r,
    was, war, w1ss, w1rs, w2ss, w2rs, wzss, wzrs, w3ss, w3rs, wbs, wbr,
):
    samples, fields, width = pooled_ref.shape
    bag = bag_ref.shape[1]
    rows = keep.shape[2]
    part1_of, part2_of = part1.shape[0] // fields, part2.shape[0] // fields
    nz, ny = size_gx // 2, size_gy // 2
    npc = 2 * ny
    gx, gy = lax.axis_index("gx"), lax.axis_index("gy")
    z, x, y, c = gx // 2, gx % 2, gy // 2, gy % 2
    spot = x * ny + y
    sibling = (gx, y * 2 + 1 - c)
    across = (z * 2 + 1 - x, gy)

    def spot_peer(d):
        to = (spot + d) % npc
        return (z * 2 + to // ny, (to % ny) * 2 + c)

    def row_peer(d):
        return (gx, ((y + d) % ny) * 2 + c)

    def far_peer(d):
        return (z * 2 + 1 - x, ((y + d) % ny) * 2 + c)

    def z_peer(d):
        return (((z + d) % nz) * 2 + x, gy)

    def z_side(up, hop=1):
        return ((z + hop if up else z - hop) * 2 + x, gy)

    def z_reaches(up, hop=1):
        return z < nz - hop if up else z >= hop

    def z_forwards(up):
        return jnp.logical_and(z_reaches(up), z >= 2 if up else z < nz - 2)

    def remote(src, dst, send, recv, dev):
        return pltpu.make_async_remote_copy(
            src_ref=src, dst_ref=dst, send_sem=send, recv_sem=recv,
            device_id=dev, device_id_type=MESH,
        )

    def m_copy(d, slot):
        return remote(notes.at[0, z], notes.at[0, slot], ms.at[0], mr.at[slot], z_peer(d))

    def ms_copy(s):
        return remote(notes.at[0, s], notes.at[1, s], ms.at[1], mr.at[nz], sibling)

    def n_copy(d, slot):
        return remote(notes_p.at[0, spot], notes_p.at[0, slot], ns.at[0], nr.at[slot], spot_peer(d))

    def ns_copy(s):
        return remote(notes_p.at[0, s], notes_p.at[1, s], ns.at[1], nr.at[npc], sibling)

    def g_copy(f, d, slot):
        return remote(
            gath_p.at[f, 0, spot], gath_p.at[f, 0, slot], gs.at[0], gr.at[f * npc + slot],
            spot_peer(d),
        )

    def gs_copy(f, s):
        return remote(
            gath_p.at[f, 0, s], gath_p.at[f, 1, s], gs.at[1], gr.at[PLANE * npc + f], sibling
        )

    def h_copy(f, d):
        at = f * (nz - 1) + d - 1
        return remote(part_z.at[at], got_z.at[at], hs.at[0], hr.at[at], z_peer(d))

    def z_copy(f, s, up, hop=1):
        kind = 0 if hop == 2 else 1 + jnp.where(s == z, 0, 1)
        return remote(
            gath.at[f - PLANE, 0, s], gath.at[f - PLANE, 0, s], zs.at[int(up), kind], zr.at[f * nz + s],
            z_side(up, hop),
        )

    def s_copy(f, s):
        return remote(gath.at[f - PLANE, 0, s], gath.at[f - PLANE, 1, s], ss.at[0], sr.at[f], sibling)

    def s_copies(f):
        return remote(gath.at[f - PLANE, 0], gath.at[f - PLANE, 1], ss.at[0], sr.at[f], sibling)

    def first_copy(f, j, dev):
        at = f * part1_of + j
        return remote(part1.at[at], got1.at[at], p1s.at[0], p1r.at[at], dev)

    def second_copy(f, j, dev):
        at = f * part2_of + j
        return remote(part2.at[at], got2.at[at], p2s.at[0], p2r.at[at], dev)

    def wa_copy():
        return remote(w0.at[pl.ds((1 - c) * npc, npc)], wsib, was.at[0], war.at[0], sibling)

    def w1_copy(d):
        return remote(w1s.at[(spot + d) % npc], w1.at[d], w1ss.at[d], w1rs.at[d], spot_peer(d))

    def w2_copy(d):
        return remote(w2s.at[(z + d) % nz], w2.at[d], w2ss.at[d], w2rs.at[d], z_peer(d))

    def wz_copy(d, slot):
        return remote(wz.at[z], wz.at[slot], wzss.at[d], wzrs.at[d], z_peer(d))

    def w3_copy(d, slot):
        return remote(
            w3.at[c * npc + spot], w3.at[slot], w3ss.at[d], w3rs.at[d], spot_peer(d)
        )

    def wb_copy(half):
        at = pl.ds(half * npc, npc)
        return remote(w3.at[at], w3.at[at], wbs.at[0], wbr.at[0], sibling)

    pairs = pair_list(fields)
    number = {pair: p for p, pair in enumerate(pairs)}
    first = [number[i, i + 1] for i in range(fields - 1)]

    def cot_load(i):
        at = pl.ds(first[i], fields - 1 - i)
        return pltpu.make_async_copy(cot_hbm.at[at], cot_ref.at[at], cs.at[i])

    loads = [
        pltpu.make_async_copy(src, dst, ls.at[n])
        for n, (src, dst) in enumerate([
            (pooled_hbm, pooled_ref), (bil_hbm, bil_ref), (bag_hbm, bag_ref),
            (lens_hbm, lens_ref), (home_hbm, home_ref),
        ])
    ]
    for n in (4, 2, 3, 0):
        loads[n].start()
    cot_load(0).start()
    loads[1].start()
    for i in range(1, fields - 1):
        cot_load(i).start()

    barrier = pltpu.get_barrier_semaphore()
    for d in range(1, nz):
        pl.semaphore_signal(barrier, inc=1, device_id=z_peer(d), device_id_type=MESH)
    for d in range(1, npc):
        pl.semaphore_signal(barrier, inc=1, device_id=spot_peer(d), device_id_type=MESH)
    pl.semaphore_signal(barrier, inc=1, device_id=sibling, device_id_type=MESH)

    def spread_out(b, carry):
        pool_f[pl.ds(pl.multiple_of(b * fields, fields), fields), :] = pooled_ref[b].astype(F32)
        return carry

    def write_notes():
        for load in loads[2:]:
            load.wait()
        bags = [bag_ref[:, k, :] for k in range(bag)]
        high = [b // LANES for b in bags]
        low = [b % LANES for b in bags]

        def look(h, found):
            row = home_ref[:, pl.ds(pl.multiple_of(h * LANES, LANES), LANES)]
            return tuple(
                jnp.where(high[k] == h, jnp.take_along_axis(row, low[k], axis=1), found[k])
                for k in range(bag)
            )

        none = jnp.full(lens_ref.shape, 0, jnp.int32)
        found = lax.fori_loop(0, home_ref.shape[1] // LANES, look, (none,) * bag, unroll=64)
        lens = lens_ref[...]
        live = [jnp.where(lens > k, found[k], -1) for k in range(bag)]
        for k in range(bag):
            times = None
            for other in live:
                same = jnp.where(live[k] == other, 1, 0)
                times = same if times is None else times + same
            note = live[k] * 8 + jnp.where(live[k] < 0, 0, times)
            notes[0, z, :, k, :] = note
            notes_p[0, spot, :, k, :] = note[:PLANE]

    write_notes()
    loads[0].wait()
    lax.fori_loop(0, samples, spread_out, 0, unroll=8)
    loads[1].wait()

    pool = lambda f: pool_f[pl.ds(f, samples, stride=fields), :]
    cot = lambda i, j: cot_ref[number[i, j]].astype(F32)
    piece, share = w0.shape[1], wz.shape[1]

    def send_own(copy, early=True):
        for hop in (2, 1):
            for up in (False, True):
                ok = z_reaches(up, hop)
                if hop == 1 and not early:
                    ok = jnp.logical_and(ok, jnp.logical_not(z_forwards(up)))

                @pl.when(ok)
                def _():
                    copy(up, hop).start()

    for i in range(fields):
        total = None
        if i < fields - 1:
            cot_load(i).wait()
            mine = pool(i).astype(BF)
            upper = jnp.zeros((samples, width), F32)
            for j in range(i + 1, fields):
                upper = upper + cot(i, j) * pool(j)
            upper = upper.astype(BF)
            total = lax.dot_general(
                upper, bil_ref[i], (((1,), (1,)), ((), ())), preferred_element_type=F32
            )
        for k in range(i):
            term = cot(k, i) * proj_f[k]
            total = term if total is None else total + term
        if i < PLANE:
            gath_p[i, 0, spot] = total.astype(BF)
        else:
            gath[i - PLANE, 0, z] = total.astype(BF)
        if i == 0:
            pl.semaphore_wait(barrier, nz - 1 + npc - 1 + 1)
            for d in range(1, nz):
                m_copy(d, z).start()
            ms_copy(z).start()
            for d in range(1, npc):
                n_copy(d, spot).start()
            ns_copy(spot).start()
        if i < PLANE:
            for d in range(npc - 1, 0, -1):
                g_copy(i, d, spot).start()
            gs_copy(i, spot).start()
        else:
            send_own(lambda up, hop: z_copy(i, z, up, hop), i < PLANE + EARLY)
            s_copy(i, z).start()
        if i < fields - 1:
            upper_b[i] = upper
            proj_f[i] = jnp.dot(mine, bil_ref[i], preferred_element_type=F32)

    def weights_here():
        for i in range(fields - 1):
            wide_w = lax.dot_general(
                pool(i).astype(BF), upper_b[i], (((0,), (0,)), ((), ())),
                preferred_element_type=F32,
            )
            at, end = i * width, (i + 1) * width
            while at < end:
                p, r = at // piece, at % piece
                n = min(piece - r, end - at)
                w0[p, r : r + n, :] = wide_w[at - i * width : at - i * width + n, :]
                at += n
        wa_copy().start()

    weights_here()

    def take(arrived, onward, to_sibling):
        for o in range(1, nz):
            for up in (True, False):
                s = z - o if up else z + o

                @pl.when(s >= 0 if up else s < nz)
                def _():
                    arrived(s)

                    if o > 1:
                        @pl.when(z_reaches(up))
                        def _():
                            onward(s, up)

                    to_sibling(s)

    def receive(f):
        take(
            lambda s: z_copy(f, s, True).wait_recv(),
            lambda s, up: z_copy(f, s, up).start(),
            lambda s: s_copy(f, s).start(),
        )
        for up in (False, True):
            @pl.when(jnp.logical_and(z_forwards(up), f + EARLY < fields))
            def _():
                z_copy(f + EARLY, z, up).start()

    for d in range(1, npc):
        s = (spot + d) % npc
        n_copy(d, s).wait_recv()
        ns_copy(s).start()
        for f in range(PLANE):
            g_copy(f, d, s).wait_recv()
            gs_copy(f, s).start()
    for d in range(1, nz):
        s = (z + d) % nz
        m_copy(d, s).wait_recv()
        ms_copy(s).start()

    steps = (
        (W1, lambda: weights_in_plane()), (W2, lambda: weights_along_z()),
        (W3, lambda: weights_back_z()), (W4, lambda: weights_back()),
        (W5, lambda: weights_to_sibling()),
    )

    row_number = lax.broadcasted_iota(jnp.int32, (rows, samples), 0).astype(F32).astype(BF)
    zero = jnp.zeros((), BF)

    def owner_of(t):
        return 1 - x if t // ny == 1 else x, (y + t % ny) % ny

    def add_half(values, note_of, sources, owners, fresh):
        group = min(GROUP, len(owners))
        for t0 in range(0, len(owners), group):
            totals = [None] * group
            for s in range(0, sources, 2):
                held = jnp.concatenate([values(s), values(s + 1)], axis=0)
                note = [note_of(s), note_of(s + 1)]
                place = [n >> 3 for n in note]
                times = [(n & 7).astype(F32).astype(BF) for n in note]
                for t in range(group):
                    z_to, x_to, y_to = owners[t0 + t]
                    base = ((z_to * 2 + x_to) * size_gy + y_to * 2 + c) * rows
                    blocks = []
                    for e in range(2):
                        key = (place[e] - base).astype(F32).astype(BF)
                        count = zero
                        for k in range(bag):
                            count = jnp.where(
                                row_number == key[k : k + 1, :], times[e][k : k + 1, :], count
                            )
                        blocks.append(count)
                    part = jnp.dot(
                        jnp.concatenate(blocks, axis=1), held, preferred_element_type=F32
                    )
                    totals[t] = part if totals[t] is None else totals[t] + part
            for t in range(group):
                sums[t0 + t] = totals[t] if fresh else sums[t0 + t] + totals[t]

    def plane_sums(f):
        owners = [((z + d) % nz, x, y) for d in range(nz)]
        for core in range(2):
            if core:
                remote(
                    gath_p.at[f, 0], gath_p.at[f, 1], gs.at[1], gr.at[PLANE * npc + f], sibling
                ).wait_recv()
            add_half(
                lambda s: gath_p[f, core, s], lambda s: notes_p[core, s, f], npc, owners,
                core == 0,
            )
        for d in range(1, nz):
            part_z[f * (nz - 1) + d - 1] = sums[d].astype(BF)
        out_ref[pl.ds(f, rows, stride=fields), :] = sums[0]

    def plane_last(f):
        at = pl.ds(f, rows, stride=fields)
        total = out_ref[at, :]
        for d in range(1, nz):
            h_copy(f, d).wait_recv()
            total = total + got_z[f * (nz - 1) + d - 1].astype(F32)
        out_ref[at, :] = total

    def by_x(f):
        return jnp.logical_and(f % 2 == 0, f < fields - DIRECT)

    def by_y(f):
        return jnp.logical_and(f % 2 == 1, f < fields - DIRECT)

    def straight(f):
        return f >= fields - DIRECT

    def field_sums(f):
        owners = [(z, *owner_of(t)) for t in range(npc)]
        for core in range(2):
            if core:
                s_copies(f).wait_recv()
            add_half(
                lambda s: gath[f - PLANE, core, s], lambda s: notes[core, s, f], nz, owners,
                core == 0,
            )

        @pl.when(by_x(f))
        def _():
            for d in range(ny):
                part1[f * part1_of + d] = sums[ny + d].astype(BF)
                first_copy(f, d, across).start()
            for d in range(1, ny):
                keep[f, d - 1] = sums[d]

        @pl.when(by_y(f))
        def _():
            for d in range(1, ny):
                part1[f * part1_of + d - 1] = sums[ny + d].astype(BF)
                first_copy(f, d - 1, row_peer(d)).start()
                part1[f * part1_of + ny + d - 2] = sums[d].astype(BF)
                first_copy(f, ny + d - 2, row_peer(d)).start()
            keep[f, 0] = sums[ny]

        @pl.when(straight(f))
        def _():
            for d in range(ny - 1, -1, -1):
                for other in (1, 0):
                    t = other * ny + d
                    if t:
                        part1[f * part1_of + t - 1] = sums[t].astype(BF)
                        dev = across if d == 0 else row_peer(d) if other == 0 else far_peer(d)
                        first_copy(f, t - 1, dev).start()

        out_ref[pl.ds(f, rows, stride=fields), :] = sums[0]

    def second_step(f):
        @pl.when(by_x(f))
        def _():
            for j in range(ny):
                first_copy(f, j, across).wait_recv()
            for d in range(1, ny):
                part2[f * part2_of + d - 1] = (keep[f, d - 1] + got1[f * part1_of + d].astype(F32)).astype(BF)
                second_copy(f, d - 1, row_peer(d)).start()

        @pl.when(by_y(f))
        def _():
            for j in range(npc - 2):
                first_copy(f, j, sibling).wait_recv()
            total = keep[f, 0]
            for j in range(ny - 1):
                total = total + got1[f * part1_of + j].astype(F32)
            part2[f * part2_of + 0] = total.astype(BF)
            second_copy(f, 0, across).start()

    def last_step(f):
        at = pl.ds(f, rows, stride=fields)

        @pl.when(by_x(f))
        def _():
            total = out_ref[at, :] + got1[f * part1_of + 0].astype(F32)
            for j in range(ny - 1):
                second_copy(f, j, sibling).wait_recv()
                total = total + got2[f * part2_of + j].astype(F32)
            out_ref[at, :] = total

        @pl.when(by_y(f))
        def _():
            total = out_ref[at, :]
            for j in range(ny - 1, npc - 2):
                total = total + got1[f * part1_of + j].astype(F32)
            second_copy(f, 0, sibling).wait_recv()
            out_ref[at, :] = total + got2[f * part2_of + 0].astype(F32)

        @pl.when(straight(f))
        def _():
            total = out_ref[at, :]
            for j in range(npc - 1):
                first_copy(f, j, sibling).wait_recv()
                total = total + got1[f * part1_of + j].astype(F32)
            out_ref[at, :] = total

    def weights_in_plane():
        wa_copy().wait_recv()
        for d in range(1, npc):
            to = (spot + d) % npc
            w1s[to] = (w0[c * npc + to] + wsib[to]).astype(BF)
            w1_copy(d).start()

    def slices(r):
        return slice(min(piece, r * share), min(piece, (r + 1) * share))

    def weights_along_z():
        total = w0[c * npc + spot] + wsib[spot]
        for d in range(1, npc):
            w1_copy(d).wait_recv()
            total = total + w1[d].astype(F32)
        for r in range(-(-piece // share)):
            rows_r = total[slices(r)]
            w2f[r, : rows_r.shape[0]] = rows_r
            w2s[r, : rows_r.shape[0]] = rows_r.astype(BF)
        for d in range(1, nz):
            w2_copy(d).start()

    def weights_back_z():
        total = w2f[z]
        for d in range(1, nz):
            w2_copy(d).wait_recv()
            total = total + w2[d].astype(F32)
        wz[z] = total.astype(BF)
        for d in range(1, nz):
            wz_copy(d, z).start()

    def weights_back():
        for d in range(1, nz):
            wz_copy(d, (z - d) % nz).wait_recv()
        for r in range(-(-piece // share)):
            at = slices(r)
            w3[c * npc + spot, at] = wz[r, : at.stop - at.start]
        for d in range(1, npc):
            w3_copy(d, c * npc + spot).start()

    def weights_to_sibling():
        for d in range(1, npc):
            w3_copy(d, c * npc + (spot - d) % npc).wait_recv()
        wb_copy(c).start()

    def early_steps(n):
        for at, step in steps:
            if at == n:
                step()

    early_steps(-2)
    if PLANE:
        remote(notes_p.at[0], notes_p.at[1], ns.at[1], nr.at[npc], sibling).wait_recv()
    for f in range(PLANE):
        plane_sums(f)
    edge = jnp.logical_or(z == 0, z == nz - 1)
    ahead = jnp.where(edge, AHEAD_END, AHEAD_MID)
    for f in range(max(AHEAD_MID, AHEAD_END)):
        @pl.when(f < ahead)
        def _():
            receive(PLANE + f)

    early_steps(-1)
    remote(notes.at[0], notes.at[1], ms.at[1], mr.at[nz], sibling).wait_recv()

    def one_field(f, carry):
        held_back = jnp.logical_and(edge, f == PLANE) if AHEAD_END else f < 0
        if AHEAD_END:
            @pl.when(jnp.logical_and(edge, f == PLANE + 1))
            def _():
                receive(f + AHEAD_END - 1)

        @pl.when(jnp.logical_and(f + ahead < fields, jnp.logical_not(held_back)))
        def _():
            receive(f + ahead)

        field_sums(f)

        for at, step in steps:
            if at >= 0:
                @pl.when(f == at)
                def _():
                    step()

        @pl.when(f == PLANE_AT)
        def _():
            for k in range(PLANE):
                for d in range(1, nz):
                    h_copy(k, d).start()

        @pl.when(f >= PLANE + LAG_SECOND)
        def _():
            second_step(f - LAG_SECOND)

        @pl.when(f >= PLANE + LAG_FINAL)
        def _():
            last_step(f - LAG_FINAL)

        return carry

    lax.fori_loop(PLANE, fields, one_field, 0)

    def late_second(f, carry):
        second_step(f)
        return carry

    lax.fori_loop(max(PLANE, fields - LAG_SECOND), fields, late_second, 0)
    for f in range(PLANE):
        plane_last(f)
    wb_copy(1 - c).wait_recv()
    wout_ref[...] = w3[...].astype(F32)

    def late_last(f, carry):
        last_step(f)
        return carry

    lax.fori_loop(max(PLANE, fields - LAG_FINAL), fields, late_last, 0)

    def sent(ref, sem):
        remote(ref, ref, sem, zr.at[0], sibling).wait_send()

    for up in (False, True):
        for hop in (1, 2):
            @pl.when(z_reaches(up, hop))
            def _():
                sent(gath.at[:, 0, 0], zs.at[int(up), 2 - hop])
        for o in range(2, nz - 1):
            @pl.when(jnp.logical_and(z_reaches(up), z >= o if up else z < nz - o))
            def _():
                sent(gath.at[:, 0, 0], zs.at[int(up), 2])
    for d in range(1, nz):
        m_copy(d, z).wait_send()
    sent(notes.at[0], ms.at[1])
    sent(gath.at[:, 0], ss.at[0])
    two_step = range(PLANE, fields - DIRECT)
    n1 = sum(ny if f % 2 == 0 else npc - 2 for f in two_step) + DIRECT * (npc - 1)
    n2 = sum(ny - 1 if f % 2 == 0 else 1 for f in two_step)
    if PLANE:
        for d in range(1, npc):
            n_copy(d, spot).wait_send()
            for f in range(PLANE):
                g_copy(f, d, spot).wait_send()
        sent(notes_p.at[0], ns.at[1])
        sent(gath_p.at[:, 0], gs.at[1])
        sent(part_z, hs.at[0])
    sent(part1.at[pl.ds(0, n1)], p1s.at[0])
    sent(part2.at[pl.ds(0, n2)], p2s.at[0])
    wa_copy().wait_send()
    wb_copy(c).wait_send()
    for d in range(1, nz):
        w2_copy(d).wait_send()
        wz_copy(d, z).wait_send()
    for d in range(1, npc):
        w1_copy(d).wait_send()
        w3_copy(d, c * npc + spot).wait_send()


def on_device(size_gx, size_gy, pooled, cotangent, bilinear, bag_ids, bag_lens, row_home):
    samples, fields, width = pooled.shape
    bag = bag_ids.shape[2]
    rows = row_home.shape[1] // (size_gx * size_gy)
    nz, ny, plane = size_gx // 2, size_gy // 2, 2 * size_gy
    npc = 2 * ny
    pairs = fields * (fields - 1) // 2
    piece = (fields - 1) * width // plane
    nb1, nb2 = npc - 1, ny - 1
    share = -(-piece // nz)
    vmem = pl.BlockSpec(memory_space=pltpu.VMEM)
    hbm = pl.BlockSpec(memory_space=pltpu.HBM)
    dma = pltpu.SemaphoreType.DMA
    buffers = [
        ((samples, fields, width), BF),
        ((pairs, samples, width), BF),
        ((fields - 1, width, width), BF),
        ((fields, bag, samples), jnp.int32),
        ((fields, samples), jnp.int32),
        (row_home.shape, jnp.int32),
        ((samples * fields, width), F32),
        ((fields - 1, samples, width), F32),
        ((fields - 1, samples, width), BF),
        ((2, nz, fields, bag, samples), jnp.int32),
        ((2, npc, PLANE, bag, samples), jnp.int32),
        ((fields - PLANE, 2, nz, samples, width), BF),
        ((PLANE, 2, npc, samples, width), BF),
        ((PLANE * (nz - 1), rows, width), BF),
        ((PLANE * (nz - 1), rows, width), BF),
        ((max(npc, nz), rows, width), F32),
        ((fields, nb2, rows, width), F32),
        ((fields * nb1, rows, width), BF),
        ((fields * nb1, rows, width), BF),
        ((fields * nb2, rows, width), BF),
        ((fields * nb2, rows, width), BF),
        ((plane, piece, width), F32),
        ((npc, piece, width), F32),
        ((npc, piece, width), BF),
        ((npc, piece, width), BF),
        ((nz, share, width), F32),
        ((nz, share, width), BF),
        ((nz, share, width), BF),
        ((nz, share, width), BF),
        ((plane, piece, width), BF),
    ]
    held = sum(math.prod(shape) * jnp.dtype(kind).itemsize for shape, kind in buffers)
    table, weight = pl.pallas_call(
        functools.partial(kernel, size_gx, size_gy),
        out_shape=(
            jax.ShapeDtypeStruct((rows * fields, width), F32),
            jax.ShapeDtypeStruct((plane, piece, width), F32),
        ),
        in_specs=[hbm] * 6,
        out_specs=(vmem,) * 2,
        scratch_shapes=[pltpu.VMEM(shape, kind) for shape, kind in buffers] + [
            dma((5,)),
            dma((fields - 1,)),
            dma((2,)),
            dma((nz + 1,)),
            dma((2,)),
            dma((npc + 1,)),
            dma((2,)),
            dma((PLANE * npc + PLANE,)),
            dma((1,)),
            dma((PLANE * (nz - 1),)),
            dma((2, 3)),
            dma((fields * nz,)),
            dma((1,)),
            dma((fields,)),
            dma((1,)),
            dma((fields * nb1,)),
            dma((1,)),
            dma((fields * nb2,)),
            dma((1,)),
            dma((1,)),
            dma((npc,)),
            dma((npc,)),
            dma((nz,)),
            dma((nz,)),
            dma((nz,)),
            dma((nz,)),
            dma((npc,)),
            dma((npc,)),
            dma((1,)),
            dma((1,)),
        ],
        compiler_params=pltpu.CompilerParams(
            collective_id=0, has_side_effects=True, vmem_limit_bytes=held + (10 << 20)
        ),
    )(*(pltpu.with_memory_space_constraint(v, pltpu.HBM) for v in (
        pooled, cotangent.transpose(1, 0, 2), bilinear,
        bag_ids.transpose(1, 2, 0), bag_lens.transpose(1, 0), row_home,
    )))
    return (
        weight.reshape(fields - 1, width, width),
        table.reshape(rows, fields, width),
    )


def solution(mesh):
    placed = (
        P(("gx", "gy"), None, None),
        P(("gx", "gy"), None, None),
        P(),
        P(("gx", "gy"), None, None),
        P(("gx", "gy"), None),
        P(),
    )
    return jax.shard_map(
        functools.partial(on_device, mesh.shape["gx"], mesh.shape["gy"]),
        mesh=mesh,
        in_specs=placed,
        out_specs=(P(), P(("gx", "gy"), None, None)),
        check_vma=False,
    )
```

```python
import functools
import math

import jax
import jax.numpy as jnp
from jax import lax
from jax.experimental import pallas as pl
from jax.experimental.pallas import tpu as pltpu
from jax.sharding import PartitionSpec as P

MESH = pl.DeviceIdType.MESH
BF = jnp.bfloat16
F32 = jnp.float32
LANES = 128
PLANE = 2
PLANE_AT = 5
GROUP = 4
EARLY = 2
W1 = -2
W2 = -1
W3 = 3
W4 = 5
W5 = 7
NOTES_AT = 2
AHEAD_END = 0
AHEAD_MID = 2
DIRECT = 1
LAG_SECOND = 2
LAG_FINAL = 8


def pair_list(fields):
    return [(i, j) for i in range(fields) for j in range(i + 1, fields)]


def kernel(
    size_gx, size_gy,
    pooled_hbm, cot_hbm, bil_hbm, bag_hbm, lens_hbm, home_hbm,
    out_ref, wout_ref,
    pooled_ref, cot_ref, bil_ref, bag_ref, lens_ref, home_ref,
    pool_f, proj_f, upper_b,
    notes, notes_p, gath, gath_p, part_z, got_z, sums, keep, part1, got1, part2, got2,
    w0, wsib, w1s, w1, w2f, w2s, w2, wz, w3,
    ls, cs,
    ms, mr, ns, nr, gs, gr, hs, hr, zs, zr, ss, sr, p1s, p1r, p2s, p2r,
    was, war, w1ss, w1rs, w2ss, w2rs, wzss, wzrs, w3ss, w3rs, wbs, wbr,
):
    samples, fields, width = pooled_ref.shape
    bag = bag_ref.shape[1]
    rows = keep.shape[2]
    part1_of, part2_of = part1.shape[0] // fields, part2.shape[0] // fields
    nz, ny = size_gx // 2, size_gy // 2
    npc = 2 * ny
    gx, gy = lax.axis_index("gx"), lax.axis_index("gy")
    z, x, y, c = gx // 2, gx % 2, gy // 2, gy % 2
    spot = x * ny + y
    sibling = (gx, y * 2 + 1 - c)
    across = (z * 2 + 1 - x, gy)

    def spot_peer(d):
        to = (spot + d) % npc
        return (z * 2 + to // ny, (to % ny) * 2 + c)

    def row_peer(d):
        return (gx, ((y + d) % ny) * 2 + c)

    def far_peer(d):
        return (z * 2 + 1 - x, ((y + d) % ny) * 2 + c)

    def z_peer(d):
        return (((z + d) % nz) * 2 + x, gy)

    def z_side(up, hop=1):
        return ((z + hop if up else z - hop) * 2 + x, gy)

    def z_reaches(up, hop=1):
        return z < nz - hop if up else z >= hop

    def z_forwards(up):
        return jnp.logical_and(z_reaches(up), z >= 2 if up else z < nz - 2)

    def remote(src, dst, send, recv, dev):
        return pltpu.make_async_remote_copy(
            src_ref=src, dst_ref=dst, send_sem=send, recv_sem=recv,
            device_id=dev, device_id_type=MESH,
        )

    def m_copy(d, slot):
        return remote(notes.at[0, z], notes.at[0, slot], ms.at[0], mr.at[slot], z_peer(d))

    def ms_copy(s):
        return remote(notes.at[0, s], notes.at[1, s], ms.at[1], mr.at[nz], sibling)

    def n_copy(d, slot):
        return remote(notes_p.at[0, spot], notes_p.at[0, slot], ns.at[0], nr.at[slot], spot_peer(d))

    def ns_copy(s):
        return remote(notes_p.at[0, s], notes_p.at[1, s], ns.at[1], nr.at[npc], sibling)

    def g_copy(f, d, slot):
        return remote(
            gath_p.at[f, 0, spot], gath_p.at[f, 0, slot], gs.at[0], gr.at[f * npc + slot],
            spot_peer(d),
        )

    def gs_copy(f, s):
        return remote(
            gath_p.at[f, 0, s], gath_p.at[f, 1, s], gs.at[1], gr.at[PLANE * npc + f], sibling
        )

    def h_copy(f, d):
        at = f * (nz - 1) + d - 1
        return remote(part_z.at[at], got_z.at[at], hs.at[0], hr.at[at], z_peer(d))

    def z_copy(f, s, up, hop=1):
        kind = 0 if hop == 2 else 1 + jnp.where(s == z, 0, 1)
        return remote(
            gath.at[f - PLANE, 0, s], gath.at[f - PLANE, 0, s], zs.at[int(up), kind], zr.at[f * nz + s],
            z_side(up, hop),
        )

    def s_copy(f, s):
        return remote(gath.at[f - PLANE, 0, s], gath.at[f - PLANE, 1, s], ss.at[0], sr.at[f], sibling)

    def s_copies(f):
        return remote(gath.at[f - PLANE, 0], gath.at[f - PLANE, 1], ss.at[0], sr.at[f], sibling)

    def first_copy(f, j, dev):
        at = f * part1_of + j
        return remote(part1.at[at], got1.at[at], p1s.at[0], p1r.at[at], dev)

    def second_copy(f, j, dev):
        at = f * part2_of + j
        return remote(part2.at[at], got2.at[at], p2s.at[0], p2r.at[at], dev)

    def wa_copy():
        return remote(w0.at[pl.ds((1 - c) * npc, npc)], wsib, was.at[0], war.at[0], sibling)

    def w1_copy(d):
        return remote(w1s.at[(spot + d) % npc], w1.at[d], w1ss.at[d], w1rs.at[d], spot_peer(d))

    def w2_copy(d):
        return remote(w2s.at[(z + d) % nz], w2.at[d], w2ss.at[d], w2rs.at[d], z_peer(d))

    def wz_copy(d, slot):
        return remote(wz.at[z], wz.at[slot], wzss.at[d], wzrs.at[d], z_peer(d))

    def w3_copy(d, slot):
        return remote(
            w3.at[c * npc + spot], w3.at[slot], w3ss.at[d], w3rs.at[d], spot_peer(d)
        )

    def wb_copy(half):
        at = pl.ds(half * npc, npc)
        return remote(w3.at[at], w3.at[at], wbs.at[0], wbr.at[0], sibling)

    pairs = pair_list(fields)
    number = {pair: p for p, pair in enumerate(pairs)}
    first = [number[i, i + 1] for i in range(fields - 1)]

    def cot_load(i):
        at = pl.ds(first[i], fields - 1 - i)
        return pltpu.make_async_copy(cot_hbm.at[at], cot_ref.at[at], cs.at[i])

    loads = [
        pltpu.make_async_copy(src, dst, ls.at[n])
        for n, (src, dst) in enumerate([
            (pooled_hbm, pooled_ref), (bil_hbm, bil_ref), (bag_hbm, bag_ref),
            (lens_hbm, lens_ref), (home_hbm, home_ref),
        ])
    ]
    loads[0].start()
    cot_load(0).start()
    for n in (1, 4, 2, 3):
        loads[n].start()
    for i in range(1, fields - 1):
        cot_load(i).start()

    barrier = pltpu.get_barrier_semaphore()
    for d in range(1, nz):
        pl.semaphore_signal(barrier, inc=1, device_id=z_peer(d), device_id_type=MESH)
    for d in range(1, npc):
        pl.semaphore_signal(barrier, inc=1, device_id=spot_peer(d), device_id_type=MESH)
    pl.semaphore_signal(barrier, inc=1, device_id=sibling, device_id_type=MESH)

    def spread_out(b, carry):
        pool_f[pl.ds(pl.multiple_of(b * fields, fields), fields), :] = pooled_ref[b].astype(F32)
        return carry

    def write_notes():
        for load in loads[2:]:
            load.wait()
        bags = [bag_ref[:, k, :] for k in range(bag)]
        high = [b // LANES for b in bags]
        low = [b % LANES for b in bags]

        def look(h, found):
            row = home_ref[:, pl.ds(pl.multiple_of(h * LANES, LANES), LANES)]
            return tuple(
                jnp.where(high[k] == h, jnp.take_along_axis(row, low[k], axis=1), found[k])
                for k in range(bag)
            )

        none = jnp.full(lens_ref.shape, 0, jnp.int32)
        found = lax.fori_loop(0, home_ref.shape[1] // LANES, look, (none,) * bag, unroll=64)
        lens = lens_ref[...]
        live = [jnp.where(lens > k, found[k], -1) for k in range(bag)]
        for k in range(bag):
            times = None
            for other in live:
                same = jnp.where(live[k] == other, 1, 0)
                times = same if times is None else times + same
            note = live[k] * 8 + jnp.where(live[k] < 0, 0, times)
            notes[0, z, :, k, :] = note
            notes_p[0, spot, :, k, :] = note[:PLANE]

    loads[0].wait()
    lax.fori_loop(0, samples, spread_out, 0, unroll=8)
    loads[1].wait()

    pool = lambda f: pool_f[pl.ds(f, samples, stride=fields), :]
    cot = lambda i, j: cot_ref[number[i, j]].astype(F32)
    piece, share = w0.shape[1], wz.shape[1]

    def send_own(copy, early=True):
        for hop in (2, 1):
            for up in (False, True):
                ok = z_reaches(up, hop)
                if hop == 1 and not early:
                    ok = jnp.logical_and(ok, jnp.logical_not(z_forwards(up)))

                @pl.when(ok)
                def _():
                    copy(up, hop).start()

    for i in range(fields):
        total = None
        if i < fields - 1:
            cot_load(i).wait()
            mine = pool(i).astype(BF)
            upper = jnp.zeros((samples, width), F32)
            for j in range(i + 1, fields):
                upper = upper + cot(i, j) * pool(j)
            upper = upper.astype(BF)
            total = lax.dot_general(
                upper, bil_ref[i], (((1,), (1,)), ((), ())), preferred_element_type=F32
            )
        for k in range(i):
            term = cot(k, i) * proj_f[k]
            total = term if total is None else total + term
        if i < PLANE:
            gath_p[i, 0, spot] = total.astype(BF)
        else:
            gath[i - PLANE, 0, z] = total.astype(BF)
        if i == 0:
            pl.semaphore_wait(barrier, nz - 1 + npc - 1 + 1)
        if i < PLANE:
            for d in range(npc - 1, 0, -1):
                g_copy(i, d, spot).start()
            gs_copy(i, spot).start()
        else:
            send_own(lambda up, hop: z_copy(i, z, up, hop), i < PLANE + EARLY)
            s_copy(i, z).start()
        if i == NOTES_AT:
            write_notes()
            for d in range(1, nz):
                m_copy(d, z).start()
            ms_copy(z).start()
            for d in range(1, npc):
                n_copy(d, spot).start()
            ns_copy(spot).start()
        if i < fields - 1:
            upper_b[i] = upper
            proj_f[i] = jnp.dot(mine, bil_ref[i], preferred_element_type=F32)

    def weights_here():
        for i in range(fields - 1):
            wide_w = lax.dot_general(
                pool(i).astype(BF), upper_b[i], (((0,), (0,)), ((), ())),
                preferred_element_type=F32,
            )
            at, end = i * width, (i + 1) * width
            while at < end:
                p, r = at // piece, at % piece
                n = min(piece - r, end - at)
                w0[p, r : r + n, :] = wide_w[at - i * width : at - i * width + n, :]
                at += n
        wa_copy().start()

    weights_here()

    def take(arrived, onward, to_sibling):
        for o in range(1, nz):
            for up in (True, False):
                s = z - o if up else z + o

                @pl.when(s >= 0 if up else s < nz)
                def _():
                    arrived(s)

                    if o > 1:
                        @pl.when(z_reaches(up))
                        def _():
                            onward(s, up)

                    to_sibling(s)

    def receive(f):
        take(
            lambda s: z_copy(f, s, True).wait_recv(),
            lambda s, up: z_copy(f, s, up).start(),
            lambda s: s_copy(f, s).start(),
        )
        for up in (False, True):
            @pl.when(jnp.logical_and(z_forwards(up), f + EARLY < fields))
            def _():
                z_copy(f + EARLY, z, up).start()

    for d in range(1, npc):
        s = (spot + d) % npc
        n_copy(d, s).wait_recv()
        ns_copy(s).start()
        for f in range(PLANE):
            g_copy(f, d, s).wait_recv()
            gs_copy(f, s).start()
    for d in range(1, nz):
        s = (z + d) % nz
        m_copy(d, s).wait_recv()
        ms_copy(s).start()

    steps = (
        (W1, lambda: weights_in_plane()), (W2, lambda: weights_along_z()),
        (W3, lambda: weights_back_z()), (W4, lambda: weights_back()),
        (W5, lambda: weights_to_sibling()),
    )

    row_number = lax.broadcasted_iota(jnp.int32, (rows, samples), 0).astype(F32).astype(BF)
    zero = jnp.zeros((), BF)

    def owner_of(t):
        return 1 - x if t // ny == 1 else x, (y + t % ny) % ny

    def add_half(values, note_of, sources, owners, fresh):
        group = min(GROUP, len(owners))
        for t0 in range(0, len(owners), group):
            totals = [None] * group
            for s in range(0, sources, 2):
                held = jnp.concatenate([values(s), values(s + 1)], axis=0)
                note = [note_of(s), note_of(s + 1)]
                place = [n >> 3 for n in note]
                times = [(n & 7).astype(F32).astype(BF) for n in note]
                for t in range(group):
                    z_to, x_to, y_to = owners[t0 + t]
                    base = ((z_to * 2 + x_to) * size_gy + y_to * 2 + c) * rows
                    blocks = []
                    for e in range(2):
                        key = (place[e] - base).astype(F32).astype(BF)
                        count = zero
                        for k in range(bag):
                            count = jnp.where(
                                row_number == key[k : k + 1, :], times[e][k : k + 1, :], count
                            )
                        blocks.append(count)
                    part = jnp.dot(
                        jnp.concatenate(blocks, axis=1), held, preferred_element_type=F32
                    )
                    totals[t] = part if totals[t] is None else totals[t] + part
            for t in range(group):
                sums[t0 + t] = totals[t] if fresh else sums[t0 + t] + totals[t]

    def plane_sums(f):
        owners = [((z + d) % nz, x, y) for d in range(nz)]
        for core in range(2):
            if core:
                remote(
                    gath_p.at[f, 0], gath_p.at[f, 1], gs.at[1], gr.at[PLANE * npc + f], sibling
                ).wait_recv()
            add_half(
                lambda s: gath_p[f, core, s], lambda s: notes_p[core, s, f], npc, owners,
                core == 0,
            )
        for d in range(1, nz):
            part_z[f * (nz - 1) + d - 1] = sums[d].astype(BF)
        out_ref[pl.ds(f, rows, stride=fields), :] = sums[0]

    def plane_last(f):
        at = pl.ds(f, rows, stride=fields)
        total = out_ref[at, :]
        for d in range(1, nz):
            h_copy(f, d).wait_recv()
            total = total + got_z[f * (nz - 1) + d - 1].astype(F32)
        out_ref[at, :] = total

    def by_x(f):
        return jnp.logical_and(f % 2 == 0, f < fields - DIRECT)

    def by_y(f):
        return jnp.logical_and(f % 2 == 1, f < fields - DIRECT)

    def straight(f):
        return f >= fields - DIRECT

    def field_sums(f):
        owners = [(z, *owner_of(t)) for t in range(npc)]
        for core in range(2):
            if core:
                s_copies(f).wait_recv()
            add_half(
                lambda s: gath[f - PLANE, core, s], lambda s: notes[core, s, f], nz, owners,
                core == 0,
            )

        @pl.when(by_x(f))
        def _():
            for d in range(ny):
                part1[f * part1_of + d] = sums[ny + d].astype(BF)
                first_copy(f, d, across).start()
            for d in range(1, ny):
                keep[f, d - 1] = sums[d]

        @pl.when(by_y(f))
        def _():
            for d in range(1, ny):
                part1[f * part1_of + d - 1] = sums[ny + d].astype(BF)
                first_copy(f, d - 1, row_peer(d)).start()
                part1[f * part1_of + ny + d - 2] = sums[d].astype(BF)
                first_copy(f, ny + d - 2, row_peer(d)).start()
            keep[f, 0] = sums[ny]

        @pl.when(straight(f))
        def _():
            for d in range(ny - 1, -1, -1):
                for other in (1, 0):
                    t = other * ny + d
                    if t:
                        part1[f * part1_of + t - 1] = sums[t].astype(BF)
                        dev = across if d == 0 else row_peer(d) if other == 0 else far_peer(d)
                        first_copy(f, t - 1, dev).start()

        out_ref[pl.ds(f, rows, stride=fields), :] = sums[0]

    def second_step(f):
        @pl.when(by_x(f))
        def _():
            for j in range(ny):
                first_copy(f, j, across).wait_recv()
            for d in range(1, ny):
                part2[f * part2_of + d - 1] = (keep[f, d - 1] + got1[f * part1_of + d].astype(F32)).astype(BF)
                second_copy(f, d - 1, row_peer(d)).start()

        @pl.when(by_y(f))
        def _():
            for j in range(npc - 2):
                first_copy(f, j, sibling).wait_recv()
            total = keep[f, 0]
            for j in range(ny - 1):
                total = total + got1[f * part1_of + j].astype(F32)
            part2[f * part2_of + 0] = total.astype(BF)
            second_copy(f, 0, across).start()

    def last_step(f):
        at = pl.ds(f, rows, stride=fields)

        @pl.when(by_x(f))
        def _():
            total = out_ref[at, :] + got1[f * part1_of + 0].astype(F32)
            for j in range(ny - 1):
                second_copy(f, j, sibling).wait_recv()
                total = total + got2[f * part2_of + j].astype(F32)
            out_ref[at, :] = total

        @pl.when(by_y(f))
        def _():
            total = out_ref[at, :]
            for j in range(ny - 1, npc - 2):
                total = total + got1[f * part1_of + j].astype(F32)
            second_copy(f, 0, sibling).wait_recv()
            out_ref[at, :] = total + got2[f * part2_of + 0].astype(F32)

        @pl.when(straight(f))
        def _():
            total = out_ref[at, :]
            for j in range(npc - 1):
                first_copy(f, j, sibling).wait_recv()
                total = total + got1[f * part1_of + j].astype(F32)
            out_ref[at, :] = total

    def weights_in_plane():
        wa_copy().wait_recv()
        for d in range(1, npc):
            to = (spot + d) % npc
            w1s[to] = (w0[c * npc + to] + wsib[to]).astype(BF)
            w1_copy(d).start()

    def slices(r):
        return slice(min(piece, r * share), min(piece, (r + 1) * share))

    def weights_along_z():
        total = w0[c * npc + spot] + wsib[spot]
        for d in range(1, npc):
            w1_copy(d).wait_recv()
            total = total + w1[d].astype(F32)
        for r in range(-(-piece // share)):
            rows_r = total[slices(r)]
            w2f[r, : rows_r.shape[0]] = rows_r
            w2s[r, : rows_r.shape[0]] = rows_r.astype(BF)
        for d in range(1, nz):
            w2_copy(d).start()

    def weights_back_z():
        total = w2f[z]
        for d in range(1, nz):
            w2_copy(d).wait_recv()
            total = total + w2[d].astype(F32)
        wz[z] = total.astype(BF)
        for d in range(1, nz):
            wz_copy(d, z).start()

    def weights_back():
        for d in range(1, nz):
            wz_copy(d, (z - d) % nz).wait_recv()
        for r in range(-(-piece // share)):
            at = slices(r)
            w3[c * npc + spot, at] = wz[r, : at.stop - at.start]
        for d in range(1, npc):
            w3_copy(d, c * npc + spot).start()

    def weights_to_sibling():
        for d in range(1, npc):
            w3_copy(d, c * npc + (spot - d) % npc).wait_recv()
        wb_copy(c).start()

    def early_steps(n):
        for at, step in steps:
            if at == n:
                step()

    early_steps(-2)
    if PLANE:
        remote(notes_p.at[0], notes_p.at[1], ns.at[1], nr.at[npc], sibling).wait_recv()
    for f in range(PLANE):
        plane_sums(f)
    edge = jnp.logical_or(z == 0, z == nz - 1)
    ahead = jnp.where(edge, AHEAD_END, AHEAD_MID)
    for f in range(max(AHEAD_MID, AHEAD_END)):
        @pl.when(f < ahead)
        def _():
            receive(PLANE + f)

    early_steps(-1)
    remote(notes.at[0], notes.at[1], ms.at[1], mr.at[nz], sibling).wait_recv()

    def one_field(f, carry):
        held_back = jnp.logical_and(edge, f == PLANE) if AHEAD_END else f < 0
        if AHEAD_END:
            @pl.when(jnp.logical_and(edge, f == PLANE + 1))
            def _():
                receive(f + AHEAD_END - 1)

        @pl.when(jnp.logical_and(f + ahead < fields, jnp.logical_not(held_back)))
        def _():
            receive(f + ahead)

        field_sums(f)

        for at, step in steps:
            if at >= 0:
                @pl.when(f == at)
                def _():
                    step()

        @pl.when(f == PLANE_AT)
        def _():
            for k in range(PLANE):
                for d in range(1, nz):
                    h_copy(k, d).start()

        @pl.when(f >= PLANE + LAG_SECOND)
        def _():
            second_step(f - LAG_SECOND)

        @pl.when(f >= PLANE + LAG_FINAL)
        def _():
            last_step(f - LAG_FINAL)

        return carry

    lax.fori_loop(PLANE, fields, one_field, 0)

    def late_second(f, carry):
        second_step(f)
        return carry

    lax.fori_loop(max(PLANE, fields - LAG_SECOND), fields, late_second, 0)
    for f in range(PLANE):
        plane_last(f)
    wb_copy(1 - c).wait_recv()
    wout_ref[...] = w3[...].astype(F32)

    def sent(ref, sem):
        remote(ref, ref, sem, zr.at[0], sibling).wait_send()

    for up in (False, True):
        for hop in (1, 2):
            @pl.when(z_reaches(up, hop))
            def _():
                sent(gath.at[:, 0, 0], zs.at[int(up), 2 - hop])
        for o in range(2, nz - 1):
            @pl.when(jnp.logical_and(z_reaches(up), z >= o if up else z < nz - o))
            def _():
                sent(gath.at[:, 0, 0], zs.at[int(up), 2])
    for d in range(1, nz):
        m_copy(d, z).wait_send()
    sent(notes.at[0], ms.at[1])
    sent(gath.at[:, 0], ss.at[0])
    if PLANE:
        for d in range(1, npc):
            n_copy(d, spot).wait_send()
            for f in range(PLANE):
                g_copy(f, d, spot).wait_send()
        sent(notes_p.at[0], ns.at[1])
        sent(gath_p.at[:, 0], gs.at[1])
        sent(part_z, hs.at[0])
    wa_copy().wait_send()
    wb_copy(c).wait_send()
    for d in range(1, nz):
        w2_copy(d).wait_send()
        wz_copy(d, z).wait_send()
    for d in range(1, npc):
        w1_copy(d).wait_send()
        w3_copy(d, c * npc + spot).wait_send()

    def late_last(f, carry):
        last_step(f)
        return carry

    lax.fori_loop(max(PLANE, fields - LAG_FINAL), fields, late_last, 0)

    two_step = range(PLANE, fields - DIRECT)
    n1 = sum(ny if f % 2 == 0 else npc - 2 for f in two_step) + DIRECT * (npc - 1)
    n2 = sum(ny - 1 if f % 2 == 0 else 1 for f in two_step)
    sent(part1.at[pl.ds(0, n1)], p1s.at[0])
    sent(part2.at[pl.ds(0, n2)], p2s.at[0])


def on_device(size_gx, size_gy, pooled, cotangent, bilinear, bag_ids, bag_lens, row_home):
    samples, fields, width = pooled.shape
    bag = bag_ids.shape[2]
    rows = row_home.shape[1] // (size_gx * size_gy)
    nz, ny, plane = size_gx // 2, size_gy // 2, 2 * size_gy
    npc = 2 * ny
    pairs = fields * (fields - 1) // 2
    piece = (fields - 1) * width // plane
    nb1, nb2 = npc - 1, ny - 1
    share = -(-piece // nz)
    vmem = pl.BlockSpec(memory_space=pltpu.VMEM)
    hbm = pl.BlockSpec(memory_space=pltpu.HBM)
    dma = pltpu.SemaphoreType.DMA
    buffers = [
        ((samples, fields, width), BF),
        ((pairs, samples, width), BF),
        ((fields - 1, width, width), BF),
        ((fields, bag, samples), jnp.int32),
        ((fields, samples), jnp.int32),
        (row_home.shape, jnp.int32),
        ((samples * fields, width), F32),
        ((fields - 1, samples, width), F32),
        ((fields - 1, samples, width), BF),
        ((2, nz, fields, bag, samples), jnp.int32),
        ((2, npc, PLANE, bag, samples), jnp.int32),
        ((fields - PLANE, 2, nz, samples, width), BF),
        ((PLANE, 2, npc, samples, width), BF),
        ((PLANE * (nz - 1), rows, width), BF),
        ((PLANE * (nz - 1), rows, width), BF),
        ((max(npc, nz), rows, width), F32),
        ((fields, nb2, rows, width), F32),
        ((fields * nb1, rows, width), BF),
        ((fields * nb1, rows, width), BF),
        ((fields * nb2, rows, width), BF),
        ((fields * nb2, rows, width), BF),
        ((plane, piece, width), F32),
        ((npc, piece, width), F32),
        ((npc, piece, width), BF),
        ((npc, piece, width), BF),
        ((nz, share, width), F32),
        ((nz, share, width), BF),
        ((nz, share, width), BF),
        ((nz, share, width), BF),
        ((plane, piece, width), BF),
    ]
    held = sum(math.prod(shape) * jnp.dtype(kind).itemsize for shape, kind in buffers)
    table, weight = pl.pallas_call(
        functools.partial(kernel, size_gx, size_gy),
        out_shape=(
            jax.ShapeDtypeStruct((rows * fields, width), F32),
            jax.ShapeDtypeStruct((plane, piece, width), F32),
        ),
        in_specs=[hbm] * 6,
        out_specs=(vmem,) * 2,
        scratch_shapes=[pltpu.VMEM(shape, kind) for shape, kind in buffers] + [
            dma((5,)),
            dma((fields - 1,)),
            dma((2,)),
            dma((nz + 1,)),
            dma((2,)),
            dma((npc + 1,)),
            dma((2,)),
            dma((PLANE * npc + PLANE,)),
            dma((1,)),
            dma((PLANE * (nz - 1),)),
            dma((2, 3)),
            dma((fields * nz,)),
            dma((1,)),
            dma((fields,)),
            dma((1,)),
            dma((fields * nb1,)),
            dma((1,)),
            dma((fields * nb2,)),
            dma((1,)),
            dma((1,)),
            dma((npc,)),
            dma((npc,)),
            dma((nz,)),
            dma((nz,)),
            dma((nz,)),
            dma((nz,)),
            dma((npc,)),
            dma((npc,)),
            dma((1,)),
            dma((1,)),
        ],
        compiler_params=pltpu.CompilerParams(
            collective_id=0, has_side_effects=True, vmem_limit_bytes=held + (10 << 20)
        ),
    )(*(pltpu.with_memory_space_constraint(v, pltpu.HBM) for v in (
        pooled, cotangent.transpose(1, 0, 2), bilinear,
        bag_ids.transpose(1, 2, 0), bag_lens.transpose(1, 0), row_home,
    )))
    return (
        weight.reshape(fields - 1, width, width),
        table.reshape(rows, fields, width),
    )


def solution(mesh):
    placed = (
        P(("gx", "gy"), None, None),
        P(("gx", "gy"), None, None),
        P(),
        P(("gx", "gy"), None, None),
        P(("gx", "gy"), None),
        P(),
    )
    return jax.shard_map(
        functools.partial(on_device, mesh.shape["gx"], mesh.shape["gy"]),
        mesh=mesh,
        in_specs=placed,
        out_specs=(P(), P(("gx", "gy"), None, None)),
        check_vma=False,
    )
```

```python
import functools
import math

import jax
import jax.numpy as jnp
from jax import lax
from jax.experimental import pallas as pl
from jax.experimental.pallas import tpu as pltpu
from jax.sharding import PartitionSpec as P

MESH = pl.DeviceIdType.MESH
BF = jnp.bfloat16
F32 = jnp.float32
LANES = 128
PLANE = 2
PLANE_AT = 5
GROUP = 4
EARLY = 3
W1 = -2
W2 = -1
W3 = 3
W4 = 5
W5 = 7
NOTES_AT = 2
AHEAD_END = 0
AHEAD_MID = 2
DIRECT = 1
LAG_SECOND = 3
LAG_FINAL = 8


def pair_list(fields):
    return [(i, j) for i in range(fields) for j in range(i + 1, fields)]


def kernel(
    size_gx, size_gy,
    pooled_hbm, cot_hbm, bil_hbm, bag_hbm, lens_hbm, home_hbm,
    out_ref, wout_ref,
    pooled_ref, cot_ref, bil_ref, bag_ref, lens_ref, home_ref,
    pool_f, proj_f, upper_b,
    notes, notes_p, gath, gath_p, part_z, got_z, sums, keep, part1, got1, part2, got2,
    w0, wsib, w1s, w1, w2f, w2s, w2, wz, w3,
    ls, cs,
    ms, mr, ns, nr, gs, gr, hs, hr, zs, zr, ss, sr, p1s, p1r, p2s, p2r,
    was, war, w1ss, w1rs, w2ss, w2rs, wzss, wzrs, w3ss, w3rs, wbs, wbr,
):
    samples, fields, width = pooled_ref.shape
    bag = bag_ref.shape[1]
    rows = keep.shape[2]
    part1_of, part2_of = part1.shape[0] // fields, part2.shape[0] // fields
    nz, ny = size_gx // 2, size_gy // 2
    npc = 2 * ny
    gx, gy = lax.axis_index("gx"), lax.axis_index("gy")
    z, x, y, c = gx // 2, gx % 2, gy // 2, gy % 2
    spot = x * ny + y
    sibling = (gx, y * 2 + 1 - c)
    across = (z * 2 + 1 - x, gy)

    def spot_peer(d):
        to = (spot + d) % npc
        return (z * 2 + to // ny, (to % ny) * 2 + c)

    def row_peer(d):
        return (gx, ((y + d) % ny) * 2 + c)

    def far_peer(d):
        return (z * 2 + 1 - x, ((y + d) % ny) * 2 + c)

    def z_peer(d):
        return (((z + d) % nz) * 2 + x, gy)

    def z_side(up, hop=1):
        return ((z + hop if up else z - hop) * 2 + x, gy)

    def z_reaches(up, hop=1):
        return z < nz - hop if up else z >= hop

    def z_forwards(up):
        return jnp.logical_and(z_reaches(up), z >= 2 if up else z < nz - 2)

    def remote(src, dst, send, recv, dev):
        return pltpu.make_async_remote_copy(
            src_ref=src, dst_ref=dst, send_sem=send, recv_sem=recv,
            device_id=dev, device_id_type=MESH,
        )

    def m_copy(d, slot):
        return remote(notes.at[0, z], notes.at[0, slot], ms.at[0], mr.at[slot], z_peer(d))

    def ms_copy(s):
        return remote(notes.at[0, s], notes.at[1, s], ms.at[1], mr.at[nz], sibling)

    def n_copy(d, slot):
        return remote(notes_p.at[0, spot], notes_p.at[0, slot], ns.at[0], nr.at[slot], spot_peer(d))

    def ns_copy(s):
        return remote(notes_p.at[0, s], notes_p.at[1, s], ns.at[1], nr.at[npc], sibling)

    def g_copy(f, d, slot):
        return remote(
            gath_p.at[f, 0, spot], gath_p.at[f, 0, slot], gs.at[0], gr.at[f * npc + slot],
            spot_peer(d),
        )

    def gs_copy(f, s):
        return remote(
            gath_p.at[f, 0, s], gath_p.at[f, 1, s], gs.at[1], gr.at[PLANE * npc + f], sibling
        )

    def h_copy(f, d):
        at = f * (nz - 1) + d - 1
        return remote(part_z.at[at], got_z.at[at], hs.at[0], hr.at[at], z_peer(d))

    def z_copy(f, s, up, hop=1):
        kind = 0 if hop == 2 else 1 + jnp.where(s == z, 0, 1)
        return remote(
            gath.at[f - PLANE, 0, s], gath.at[f - PLANE, 0, s], zs.at[int(up), kind], zr.at[f * nz + s],
            z_side(up, hop),
        )

    def s_copy(f, s):
        return remote(gath.at[f - PLANE, 0, s], gath.at[f - PLANE, 1, s], ss.at[0], sr.at[f], sibling)

    def s_copies(f):
        return remote(gath.at[f - PLANE, 0], gath.at[f - PLANE, 1], ss.at[0], sr.at[f], sibling)

    def first_copy(f, j, dev):
        at = f * part1_of + j
        return remote(part1.at[at], got1.at[at], p1s.at[0], p1r.at[at], dev)

    def second_copy(f, j, dev):
        at = f * part2_of + j
        return remote(part2.at[at], got2.at[at], p2s.at[0], p2r.at[at], dev)

    def wa_copy():
        return remote(w0.at[pl.ds((1 - c) * npc, npc)], wsib, was.at[0], war.at[0], sibling)

    def w1_copy(d):
        return remote(w1s.at[(spot + d) % npc], w1.at[d], w1ss.at[d], w1rs.at[d], spot_peer(d))

    def w2_copy(d):
        return remote(w2s.at[(z + d) % nz], w2.at[d], w2ss.at[d], w2rs.at[d], z_peer(d))

    def wz_copy(d, slot):
        return remote(wz.at[z], wz.at[slot], wzss.at[d], wzrs.at[d], z_peer(d))

    def w3_copy(d, slot):
        return remote(
            w3.at[c * npc + spot], w3.at[slot], w3ss.at[d], w3rs.at[d], spot_peer(d)
        )

    def wb_copy(half):
        at = pl.ds(half * npc, npc)
        return remote(w3.at[at], w3.at[at], wbs.at[0], wbr.at[0], sibling)

    pairs = pair_list(fields)
    number = {pair: p for p, pair in enumerate(pairs)}
    first = [number[i, i + 1] for i in range(fields - 1)]

    def cot_load(i):
        at = pl.ds(first[i], fields - 1 - i)
        return pltpu.make_async_copy(cot_hbm.at[at], cot_ref.at[at], cs.at[i])

    loads = [
        pltpu.make_async_copy(src, dst, ls.at[n])
        for n, (src, dst) in enumerate([
            (pooled_hbm, pooled_ref), (bil_hbm, bil_ref), (bag_hbm, bag_ref),
            (lens_hbm, lens_ref), (home_hbm, home_ref),
        ])
    ]
    loads[0].start()
    cot_load(0).start()
    for n in (1, 4, 2, 3):
        loads[n].start()
    for i in range(1, fields - 1):
        cot_load(i).start()

    barrier = pltpu.get_barrier_semaphore()
    for d in range(1, nz):
        pl.semaphore_signal(barrier, inc=1, device_id=z_peer(d), device_id_type=MESH)
    for d in range(1, npc):
        pl.semaphore_signal(barrier, inc=1, device_id=spot_peer(d), device_id_type=MESH)
    pl.semaphore_signal(barrier, inc=1, device_id=sibling, device_id_type=MESH)

    def spread_out(b, carry):
        pool_f[pl.ds(pl.multiple_of(b * fields, fields), fields), :] = pooled_ref[b].astype(F32)
        return carry

    def write_notes():
        for load in loads[2:]:
            load.wait()
        bags = [bag_ref[:, k, :] for k in range(bag)]
        high = [b // LANES for b in bags]
        low = [b % LANES for b in bags]

        def look(h, found):
            row = home_ref[:, pl.ds(pl.multiple_of(h * LANES, LANES), LANES)]
            return tuple(
                jnp.where(high[k] == h, jnp.take_along_axis(row, low[k], axis=1), found[k])
                for k in range(bag)
            )

        none = jnp.full(lens_ref.shape, 0, jnp.int32)
        found = lax.fori_loop(0, home_ref.shape[1] // LANES, look, (none,) * bag, unroll=64)
        lens = lens_ref[...]
        live = [jnp.where(lens > k, found[k], -1) for k in range(bag)]
        for k in range(bag):
            times = None
            for other in live:
                same = jnp.where(live[k] == other, 1, 0)
                times = same if times is None else times + same
            note = live[k] * 8 + jnp.where(live[k] < 0, 0, times)
            notes[0, z, :, k, :] = note
            notes_p[0, spot, :, k, :] = note[:PLANE]

    loads[0].wait()
    lax.fori_loop(0, samples, spread_out, 0, unroll=8)
    loads[1].wait()

    pool = lambda f: pool_f[pl.ds(f, samples, stride=fields), :]
    cot = lambda i, j: cot_ref[number[i, j]].astype(F32)
    piece, share = w0.shape[1], wz.shape[1]

    def send_own(copy, early=True):
        for hop in (2, 1):
            for up in (False, True):
                ok = z_reaches(up, hop)
                if hop == 1 and not early:
                    ok = jnp.logical_and(ok, jnp.logical_not(z_forwards(up)))

                @pl.when(ok)
                def _():
                    copy(up, hop).start()

    for i in range(fields):
        total = None
        if i < fields - 1:
            cot_load(i).wait()
            mine = pool(i).astype(BF)
            upper = jnp.zeros((samples, width), F32)
            for j in range(i + 1, fields):
                upper = upper + cot(i, j) * pool(j)
            upper = upper.astype(BF)
            total = lax.dot_general(
                upper, bil_ref[i], (((1,), (1,)), ((), ())), preferred_element_type=F32
            )
        for k in range(i):
            term = cot(k, i) * proj_f[k]
            total = term if total is None else total + term
        if i < PLANE:
            gath_p[i, 0, spot] = total.astype(BF)
        else:
            gath[i - PLANE, 0, z] = total.astype(BF)
        if i == 0:
            pl.semaphore_wait(barrier, nz - 1 + npc - 1 + 1)
        if i < PLANE:
            for d in range(npc - 1, 0, -1):
                g_copy(i, d, spot).start()
            gs_copy(i, spot).start()
        else:
            send_own(lambda up, hop: z_copy(i, z, up, hop), i < PLANE + EARLY)
            s_copy(i, z).start()
        if i == NOTES_AT:
            write_notes()
            for d in range(1, nz):
                m_copy(d, z).start()
            ms_copy(z).start()
            for d in range(1, npc):
                n_copy(d, spot).start()
            ns_copy(spot).start()
        if i < fields - 1:
            upper_b[i] = upper
            proj_f[i] = jnp.dot(mine, bil_ref[i], preferred_element_type=F32)

    def weights_here():
        for i in range(fields - 1):
            wide_w = lax.dot_general(
                pool(i).astype(BF), upper_b[i], (((0,), (0,)), ((), ())),
                preferred_element_type=F32,
            )
            at, end = i * width, (i + 1) * width
            while at < end:
                p, r = at // piece, at % piece
                n = min(piece - r, end - at)
                w0[p, r : r + n, :] = wide_w[at - i * width : at - i * width + n, :]
                at += n
        wa_copy().start()

    weights_here()

    def take(arrived, onward, to_sibling):
        for o in range(1, nz):
            for up in (True, False):
                s = z - o if up else z + o

                @pl.when(s >= 0 if up else s < nz)
                def _():
                    arrived(s)

                    if o > 1:
                        @pl.when(z_reaches(up))
                        def _():
                            onward(s, up)

                    to_sibling(s)

    def receive(f):
        take(
            lambda s: z_copy(f, s, True).wait_recv(),
            lambda s, up: z_copy(f, s, up).start(),
            lambda s: s_copy(f, s).start(),
        )
        for up in (False, True):
            @pl.when(jnp.logical_and(z_forwards(up), f + EARLY < fields))
            def _():
                z_copy(f + EARLY, z, up).start()

    for d in range(1, npc):
        s = (spot + d) % npc
        n_copy(d, s).wait_recv()
        ns_copy(s).start()
        for f in range(PLANE):
            g_copy(f, d, s).wait_recv()
            gs_copy(f, s).start()
    for d in range(1, nz):
        s = (z + d) % nz
        m_copy(d, s).wait_recv()
        ms_copy(s).start()

    steps = (
        (W1, lambda: weights_in_plane()), (W2, lambda: weights_along_z()),
        (W3, lambda: weights_back_z()), (W4, lambda: weights_back()),
        (W5, lambda: weights_to_sibling()),
    )

    row_number = lax.broadcasted_iota(jnp.int32, (rows, samples), 0).astype(F32).astype(BF)
    zero = jnp.zeros((), BF)

    def owner_of(t):
        return 1 - x if t // ny == 1 else x, (y + t % ny) % ny

    def add_half(values, note_of, sources, owners, fresh):
        group = min(GROUP, len(owners))
        for t0 in range(0, len(owners), group):
            totals = [None] * group
            for s in range(0, sources, 2):
                held = jnp.concatenate([values(s), values(s + 1)], axis=0)
                note = [note_of(s), note_of(s + 1)]
                place = [n >> 3 for n in note]
                times = [(n & 7).astype(F32).astype(BF) for n in note]
                for t in range(group):
                    z_to, x_to, y_to = owners[t0 + t]
                    base = ((z_to * 2 + x_to) * size_gy + y_to * 2 + c) * rows
                    blocks = []
                    for e in range(2):
                        key = (place[e] - base).astype(F32).astype(BF)
                        count = zero
                        for k in range(bag):
                            count = jnp.where(
                                row_number == key[k : k + 1, :], times[e][k : k + 1, :], count
                            )
                        blocks.append(count)
                    part = jnp.dot(
                        jnp.concatenate(blocks, axis=1), held, preferred_element_type=F32
                    )
                    totals[t] = part if totals[t] is None else totals[t] + part
            for t in range(group):
                sums[t0 + t] = totals[t] if fresh else sums[t0 + t] + totals[t]

    def plane_sums(f):
        owners = [((z + d) % nz, x, y) for d in range(nz)]
        for core in range(2):
            if core:
                remote(
                    gath_p.at[f, 0], gath_p.at[f, 1], gs.at[1], gr.at[PLANE * npc + f], sibling
                ).wait_recv()
            add_half(
                lambda s: gath_p[f, core, s], lambda s: notes_p[core, s, f], npc, owners,
                core == 0,
            )
        for d in range(1, nz):
            part_z[f * (nz - 1) + d - 1] = sums[d].astype(BF)
        out_ref[pl.ds(f, rows, stride=fields), :] = sums[0]

    def plane_last(f):
        at = pl.ds(f, rows, stride=fields)
        total = out_ref[at, :]
        for d in range(1, nz):
            h_copy(f, d).wait_recv()
            total = total + got_z[f * (nz - 1) + d - 1].astype(F32)
        out_ref[at, :] = total

    def by_x(f):
        return jnp.logical_and(f % 2 == 0, f < fields - DIRECT)

    def by_y(f):
        return jnp.logical_and(f % 2 == 1, f < fields - DIRECT)

    def straight(f):
        return f >= fields - DIRECT

    def field_sums(f):
        owners = [(z, *owner_of(t)) for t in range(npc)]
        for core in range(2):
            if core:
                s_copies(f).wait_recv()
            add_half(
                lambda s: gath[f - PLANE, core, s], lambda s: notes[core, s, f], nz, owners,
                core == 0,
            )

        @pl.when(by_x(f))
        def _():
            for d in range(ny):
                part1[f * part1_of + d] = sums[ny + d].astype(BF)
                first_copy(f, d, across).start()
            for d in range(1, ny):
                keep[f, d - 1] = sums[d]

        @pl.when(by_y(f))
        def _():
            for d in range(1, ny):
                part1[f * part1_of + d - 1] = sums[ny + d].astype(BF)
                first_copy(f, d - 1, row_peer(d)).start()
                part1[f * part1_of + ny + d - 2] = sums[d].astype(BF)
                first_copy(f, ny + d - 2, row_peer(d)).start()
            keep[f, 0] = sums[ny]

        @pl.when(straight(f))
        def _():
            for d in range(ny - 1, -1, -1):
                for other in (1, 0):
                    t = other * ny + d
                    if t:
                        part1[f * part1_of + t - 1] = sums[t].astype(BF)
                        dev = across if d == 0 else row_peer(d) if other == 0 else far_peer(d)
                        first_copy(f, t - 1, dev).start()

        out_ref[pl.ds(f, rows, stride=fields), :] = sums[0]

    def second_step(f):
        @pl.when(by_x(f))
        def _():
            for j in range(ny):
                first_copy(f, j, across).wait_recv()
            for d in range(1, ny):
                part2[f * part2_of + d - 1] = (keep[f, d - 1] + got1[f * part1_of + d].astype(F32)).astype(BF)
                second_copy(f, d - 1, row_peer(d)).start()

        @pl.when(by_y(f))
        def _():
            for j in range(npc - 2):
                first_copy(f, j, sibling).wait_recv()
            total = keep[f, 0]
            for j in range(ny - 1):
                total = total + got1[f * part1_of + j].astype(F32)
            part2[f * part2_of + 0] = total.astype(BF)
            second_copy(f, 0, across).start()

    def last_step(f):
        at = pl.ds(f, rows, stride=fields)

        @pl.when(by_x(f))
        def _():
            total = out_ref[at, :] + got1[f * part1_of + 0].astype(F32)
            for j in range(ny - 1):
                second_copy(f, j, sibling).wait_recv()
                total = total + got2[f * part2_of + j].astype(F32)
            out_ref[at, :] = total

        @pl.when(by_y(f))
        def _():
            total = out_ref[at, :]
            for j in range(ny - 1, npc - 2):
                total = total + got1[f * part1_of + j].astype(F32)
            second_copy(f, 0, sibling).wait_recv()
            out_ref[at, :] = total + got2[f * part2_of + 0].astype(F32)

        @pl.when(straight(f))
        def _():
            total = out_ref[at, :]
            for j in range(npc - 1):
                first_copy(f, j, sibling).wait_recv()
                total = total + got1[f * part1_of + j].astype(F32)
            out_ref[at, :] = total

    def weights_in_plane():
        wa_copy().wait_recv()
        for d in range(1, npc):
            to = (spot + d) % npc
            w1s[to] = (w0[c * npc + to] + wsib[to]).astype(BF)
            w1_copy(d).start()

    def slices(r):
        return slice(min(piece, r * share), min(piece, (r + 1) * share))

    def weights_along_z():
        total = w0[c * npc + spot] + wsib[spot]
        for d in range(1, npc):
            w1_copy(d).wait_recv()
            total = total + w1[d].astype(F32)
        for r in range(-(-piece // share)):
            rows_r = total[slices(r)]
            w2f[r, : rows_r.shape[0]] = rows_r
            w2s[r, : rows_r.shape[0]] = rows_r.astype(BF)
        for d in range(1, nz):
            w2_copy(d).start()

    def weights_back_z():
        total = w2f[z]
        for d in range(1, nz):
            w2_copy(d).wait_recv()
            total = total + w2[d].astype(F32)
        wz[z] = total.astype(BF)
        for d in range(1, nz):
            wz_copy(d, z).start()

    def weights_back():
        for d in range(1, nz):
            wz_copy(d, (z - d) % nz).wait_recv()
        for r in range(-(-piece // share)):
            at = slices(r)
            w3[c * npc + spot, at] = wz[r, : at.stop - at.start]
        for d in range(1, npc):
            w3_copy(d, c * npc + spot).start()

    def weights_to_sibling():
        for d in range(1, npc):
            w3_copy(d, c * npc + (spot - d) % npc).wait_recv()
        wb_copy(c).start()

    def early_steps(n):
        for at, step in steps:
            if at == n:
                step()

    early_steps(-2)
    if PLANE:
        remote(notes_p.at[0], notes_p.at[1], ns.at[1], nr.at[npc], sibling).wait_recv()
    for f in range(PLANE):
        plane_sums(f)
    edge = jnp.logical_or(z == 0, z == nz - 1)
    ahead = jnp.where(edge, AHEAD_END, AHEAD_MID)
    for f in range(max(AHEAD_MID, AHEAD_END)):
        @pl.when(f < ahead)
        def _():
            receive(PLANE + f)

    early_steps(-1)
    remote(notes.at[0], notes.at[1], ms.at[1], mr.at[nz], sibling).wait_recv()

    def one_field(f, carry):
        held_back = jnp.logical_and(edge, f == PLANE) if AHEAD_END else f < 0
        if AHEAD_END:
            @pl.when(jnp.logical_and(edge, f == PLANE + 1))
            def _():
                receive(f + AHEAD_END - 1)

        @pl.when(jnp.logical_and(f + ahead < fields, jnp.logical_not(held_back)))
        def _():
            receive(f + ahead)

        field_sums(f)

        for at, step in steps:
            if at >= 0:
                @pl.when(f == at)
                def _():
                    step()

        @pl.when(f == PLANE_AT)
        def _():
            for k in range(PLANE):
                for d in range(1, nz):
                    h_copy(k, d).start()

        @pl.when(f >= PLANE + LAG_SECOND)
        def _():
            second_step(f - LAG_SECOND)

        @pl.when(f >= PLANE + LAG_FINAL)
        def _():
            last_step(f - LAG_FINAL)

        return carry

    lax.fori_loop(PLANE, fields, one_field, 0)

    def late_second(f, carry):
        second_step(f)
        return carry

    lax.fori_loop(max(PLANE, fields - LAG_SECOND), fields, late_second, 0)
    for f in range(PLANE):
        plane_last(f)
    wb_copy(1 - c).wait_recv()
    wout_ref[...] = w3[...].astype(F32)

    def sent(ref, sem):
        remote(ref, ref, sem, zr.at[0], sibling).wait_send()

    for up in (False, True):
        for hop in (1, 2):
            @pl.when(z_reaches(up, hop))
            def _():
                sent(gath.at[:, 0, 0], zs.at[int(up), 2 - hop])
        for o in range(2, nz - 1):
            @pl.when(jnp.logical_and(z_reaches(up), z >= o if up else z < nz - o))
            def _():
                sent(gath.at[:, 0, 0], zs.at[int(up), 2])
    for d in range(1, nz):
        m_copy(d, z).wait_send()
    sent(notes.at[0], ms.at[1])
    sent(gath.at[:, 0], ss.at[0])
    if PLANE:
        for d in range(1, npc):
            n_copy(d, spot).wait_send()
            for f in range(PLANE):
                g_copy(f, d, spot).wait_send()
        sent(notes_p.at[0], ns.at[1])
        sent(gath_p.at[:, 0], gs.at[1])
        sent(part_z, hs.at[0])
    wa_copy().wait_send()
    wb_copy(c).wait_send()
    for d in range(1, nz):
        w2_copy(d).wait_send()
        wz_copy(d, z).wait_send()
    for d in range(1, npc):
        w1_copy(d).wait_send()
        w3_copy(d, c * npc + spot).wait_send()

    def late_last(f, carry):
        last_step(f)
        return carry

    lax.fori_loop(max(PLANE, fields - LAG_FINAL), fields, late_last, 0)

    two_step = range(PLANE, fields - DIRECT)
    n1 = sum(ny if f % 2 == 0 else npc - 2 for f in two_step) + DIRECT * (npc - 1)
    n2 = sum(ny - 1 if f % 2 == 0 else 1 for f in two_step)
    sent(part1.at[pl.ds(0, n1)], p1s.at[0])
    sent(part2.at[pl.ds(0, n2)], p2s.at[0])


def on_device(size_gx, size_gy, pooled, cotangent, bilinear, bag_ids, bag_lens, row_home):
    samples, fields, width = pooled.shape
    bag = bag_ids.shape[2]
    rows = row_home.shape[1] // (size_gx * size_gy)
    nz, ny, plane = size_gx // 2, size_gy // 2, 2 * size_gy
    npc = 2 * ny
    pairs = fields * (fields - 1) // 2
    piece = (fields - 1) * width // plane
    nb1, nb2 = npc - 1, ny - 1
    share = -(-piece // nz)
    vmem = pl.BlockSpec(memory_space=pltpu.VMEM)
    hbm = pl.BlockSpec(memory_space=pltpu.HBM)
    dma = pltpu.SemaphoreType.DMA
    buffers = [
        ((samples, fields, width), BF),
        ((pairs, samples, width), BF),
        ((fields - 1, width, width), BF),
        ((fields, bag, samples), jnp.int32),
        ((fields, samples), jnp.int32),
        (row_home.shape, jnp.int32),
        ((samples * fields, width), F32),
        ((fields - 1, samples, width), F32),
        ((fields - 1, samples, width), BF),
        ((2, nz, fields, bag, samples), jnp.int32),
        ((2, npc, PLANE, bag, samples), jnp.int32),
        ((fields - PLANE, 2, nz, samples, width), BF),
        ((PLANE, 2, npc, samples, width), BF),
        ((PLANE * (nz - 1), rows, width), BF),
        ((PLANE * (nz - 1), rows, width), BF),
        ((max(npc, nz), rows, width), F32),
        ((fields, nb2, rows, width), F32),
        ((fields * nb1, rows, width), BF),
        ((fields * nb1, rows, width), BF),
        ((fields * nb2, rows, width), BF),
        ((fields * nb2, rows, width), BF),
        ((plane, piece, width), F32),
        ((npc, piece, width), F32),
        ((npc, piece, width), BF),
        ((npc, piece, width), BF),
        ((nz, share, width), F32),
        ((nz, share, width), BF),
        ((nz, share, width), BF),
        ((nz, share, width), BF),
        ((plane, piece, width), BF),
    ]
    held = sum(math.prod(shape) * jnp.dtype(kind).itemsize for shape, kind in buffers)
    table, weight = pl.pallas_call(
        functools.partial(kernel, size_gx, size_gy),
        out_shape=(
            jax.ShapeDtypeStruct((rows * fields, width), F32),
            jax.ShapeDtypeStruct((plane, piece, width), F32),
        ),
        in_specs=[hbm] * 6,
        out_specs=(vmem,) * 2,
        scratch_shapes=[pltpu.VMEM(shape, kind) for shape, kind in buffers] + [
            dma((5,)),
            dma((fields - 1,)),
            dma((2,)),
            dma((nz + 1,)),
            dma((2,)),
            dma((npc + 1,)),
            dma((2,)),
            dma((PLANE * npc + PLANE,)),
            dma((1,)),
            dma((PLANE * (nz - 1),)),
            dma((2, 3)),
            dma((fields * nz,)),
            dma((1,)),
            dma((fields,)),
            dma((1,)),
            dma((fields * nb1,)),
            dma((1,)),
            dma((fields * nb2,)),
            dma((1,)),
            dma((1,)),
            dma((npc,)),
            dma((npc,)),
            dma((nz,)),
            dma((nz,)),
            dma((nz,)),
            dma((nz,)),
            dma((npc,)),
            dma((npc,)),
            dma((1,)),
            dma((1,)),
        ],
        compiler_params=pltpu.CompilerParams(
            collective_id=0, has_side_effects=True, vmem_limit_bytes=held + (10 << 20)
        ),
    )(*(pltpu.with_memory_space_constraint(v, pltpu.HBM) for v in (
        pooled, cotangent.transpose(1, 0, 2), bilinear,
        bag_ids.transpose(1, 2, 0), bag_lens.transpose(1, 0), row_home,
    )))
    return (
        weight.reshape(fields - 1, width, width),
        table.reshape(rows, fields, width),
    )


def solution(mesh):
    placed = (
        P(("gx", "gy"), None, None),
        P(("gx", "gy"), None, None),
        P(),
        P(("gx", "gy"), None, None),
        P(("gx", "gy"), None),
        P(),
    )
    return jax.shard_map(
        functools.partial(on_device, mesh.shape["gx"], mesh.shape["gy"]),
        mesh=mesh,
        in_specs=placed,
        out_specs=(P(), P(("gx", "gy"), None, None)),
        check_vma=False,
    )
```
